32 devices in a mesh: dp: 16 (over z, x, core), tensor: 2 (over y).
Axes of the slice: x: 2, y: 2, z: 4, core: 2. Of those that a mesh axis runs over, the one named last changes fastest.
Arguments:
- tokens: bfloat16 [8192, 1152], P(('dp', 'tensor')), may hold values from -6 to 6
- cotangent: bfloat16 [8192, 1152], P(('dp', 'tensor')), may hold values from -6 to 6
- lengths: int32 [16, 2], P('dp'), may hold values from 128 to 384, as said below
- grid_width: int32 [16, 2], P('dp'), may hold values from 4 to 32
- timestep: int32 [16, 2], P('dp'), may hold values from 0 to 999
- class_id: int32 [16, 2], P('dp'), may hold values from 0 to 999
- class_table: bfloat16 [1000, 1152], replicated, may hold values from -6 to 6
- ada_weight: float32 [1152, 6, 1152], P('dp', None, 'tensor'), may hold values from -0.1875 to 0.1875
- ada_m: float32 [1152, 6, 1152], P('dp', None, 'tensor'), may hold values from -1.5 to 1.5
- ada_v: float32 [1152, 6, 1152], P('dp', None, 'tensor'), may hold values from 0.04308992 to 0.172032
- ada_bias: float32 [6, 1152], replicated, may hold values from -3 to 3
- bias_m: float32 [6, 1152], replicated, may hold values from -1.5 to 1.5
- bias_v: float32 [6, 1152], replicated, may hold values from 0.04308992 to 0.172032
- qkv_weight: float32 [1152, 3, 1152], P('dp', None, 'tensor'), may hold values from -0.1875 to 0.1875
- qkv_m: float32 [1152, 3, 1152], P('dp', None, 'tensor'), may hold values from -1.5 to 1.5
- qkv_v: float32 [1152, 3, 1152], P('dp', None, 'tensor'), may hold values from 0.04308992 to 0.172032
- out_weight: float32 [1152, 1152], P('dp', 'tensor'), may hold values from -1.5 to 1.5
- out_m: float32 [1152, 1152], P('dp', 'tensor'), may hold values from -1.5 to 1.5
- out_v: float32 [1152, 1152], P('dp', 'tensor'), may hold values from 0.04308992 to 0.172032
- gateup_weight: float32 [1152, 2, 3072], P('dp', None, 'tensor'), may hold values from -0.1875 to 0.1875
- gateup_m: float32 [1152, 2, 3072], P('dp', None, 'tensor'), may hold values from -1.5 to 1.5
- gateup_v: float32 [1152, 2, 3072], P('dp', None, 'tensor'), may hold values from 0.04308992 to 0.172032
- down_weight: float32 [1152, 3072], P('dp', 'tensor'), may hold values from -0.109375 to 0.109375
- down_m: float32 [1152, 3072], P('dp', 'tensor'), may hold values from -1.5 to 1.5
- down_v: float32 [1152, 3072], P('dp', 'tensor'), may hold values from 0.04308992 to 0.172032
- qk_gain: float32 [2, 72], replicated, may hold values from 0.25 to 1.75
- gain_m: float32 [2, 72], replicated, may hold values from -3 to 3
- gain_v: float32 [2, 72], replicated, may hold values from 0.172032 to 0.69632
Outputs:
- out_tokens: bfloat16 [8192, 1152], P(('dp', 'tensor'))
- input_grad: bfloat16 [8192, 1152], P(('dp', 'tensor'))
- grad_norm: float32 [], replicated
- new_ada_weight: float32 [1152, 6, 1152], P('dp', None, 'tensor')
- new_ada_m: float32 [1152, 6, 1152], P('dp', None, 'tensor')
- new_ada_v: float32 [1152, 6, 1152], P('dp', None, 'tensor')
- new_ada_bias: float32 [6, 1152], replicated
- new_bias_m: float32 [6, 1152], replicated
- new_bias_v: float32 [6, 1152], replicated
- new_qkv_weight: float32 [1152, 3, 1152], P('dp', None, 'tensor')
- new_qkv_m: float32 [1152, 3, 1152], P('dp', None, 'tensor')
- new_qkv_v: float32 [1152, 3, 1152], P('dp', None, 'tensor')
- new_out_weight: float32 [1152, 1152], P('dp', 'tensor')
- new_out_m: float32 [1152, 1152], P('dp', 'tensor')
- new_out_v: float32 [1152, 1152], P('dp', 'tensor')
- new_gateup_weight: float32 [1152, 2, 3072], P('dp', None, 'tensor')
- new_gateup_m: float32 [1152, 2, 3072], P('dp', None, 'tensor')
- new_gateup_v: float32 [1152, 2, 3072], P('dp', None, 'tensor')
- new_down_weight: float32 [1152, 3072], P('dp', 'tensor')
- new_down_m: float32 [1152, 3072], P('dp', 'tensor')
- new_down_v: float32 [1152, 3072], P('dp', 'tensor')
- new_qk_gain: float32 [2, 72], replicated
- new_gain_m: float32 [2, 72], replicated
- new_gain_v: float32 [2, 72], replicated
The draws below stay inside these ranges and needn't reach their ends.
Inputs may be any that keep to these rules, and one draw needn't show every extreme that they name: Each row holds the lengths of one group's items in row order; they sum to 512, each is at most 384, and some row holds an item of exactly 384. `grid_width`: an item's patches fill its grid row by row.
All inputs are finite; a program needn't handle non-finite values.
Results may differ from the reference program's by a relative error of at most 0.015.
Values may be sent and summed in bfloat16 or wider, within the bound.
No kernel may reach another device: no remote copies, remote signals or barrier semaphores. Data moves between devices by JAX's collectives and lax.ppermute only.
A program may use at most 192 MiB of HBM per device.

```python
import math
from functools import partial
import jax
import jax.numpy as jnp
from jax import lax

D = 1152
HEADS = 16
HD = 72
FF = 3072
CLASSES = 1000
ITEMS = 2
STEP = 10
GROUP_TOK = 512
TOKENS = 8192
LONGEST = 384
QBLOCK = 512
PARAMS = 23894928
N_DP = 16


def draw_lengths(key, part):
    key_first = jax.random.fold_in(key, 11)
    key_pick = jax.random.fold_in(key, 12)
    key_order = jax.random.fold_in(key, 13)
    first_len = jax.random.randint(key_first, (N_DP,), GROUP_TOK - LONGEST, LONGEST + 1).astype(jnp.int32)
    chosen = jax.random.randint(key_pick, (), 0, N_DP).astype(jnp.int32)
    first_len = jnp.where(jnp.arange(N_DP, dtype=jnp.int32) == chosen, LONGEST, first_len).astype(jnp.int32)
    second_len = (GROUP_TOK - first_len).astype(jnp.int32)
    swapped = jax.random.randint(key_order, (N_DP,), 0, 2).astype(jnp.int32)
    lead = jnp.where(swapped == 1, second_len, first_len).astype(jnp.int32)
    trail = jnp.where(swapped == 1, first_len, second_len).astype(jnp.int32)
    return jnp.stack([lead, trail], axis=1).astype(jnp.int32)


def plant(array, stream_key, least, high):
    spot = [jax.random.randint(jax.random.fold_in(stream_key, axis), (), 0, length) for axis, length in enumerate(array.shape)]
    main_axis = array.shape.index(max(array.shape))
    next_to = spot[:main_axis] + [(spot[main_axis] + 1) % array.shape[main_axis]] + spot[main_axis + 1:]
    return array.at[tuple(spot)].set(least).at[tuple(next_to)].set(high)


def block_levels(key, shape, shards, least, top_value):
    level, own = 1.0, jax.random.fold_in(key, 6)
    for dim, parts in shards:
        draws = jnp.exp(jax.random.uniform(jax.random.fold_in(own, dim), (parts,), jnp.float32, least / len(shards), top_value / len(shards)))
        level = level * jnp.repeat(draws, shape[dim] // parts).reshape([-1 if axis == dim else 1 for axis in range(len(shape))])
    return level


def normal_values(stream_key, shape, scale, bound, split=(), held_as=jnp.bfloat16):
    array = jax.random.normal(stream_key, shape, jnp.float32) * scale
    if len(split) > 0:
        array = block_levels(stream_key, shape, split, -0.22, 0.18) * array
    return jnp.clip(array, min=-bound, max=bound).astype(held_as)


def setup_inputs(seed: int = 0) -> dict:
    streams_of = jax.random.split(jax.random.key(seed), 29)
    return {
        "tokens": normal_values(streams_of[0], (TOKENS, D), 1.0, 6.0, ((0, 32),)),
        "cotangent": normal_values(streams_of[1], (TOKENS, D), 1.0, 6.0, ((0, 32),)),
        "lengths": draw_lengths(jax.random.fold_in(streams_of[28], 71), 0),
        "grid_width": plant(jax.random.randint(streams_of[3], (N_DP, ITEMS), 4, 33), jax.random.fold_in(streams_of[3], 1), 4, 32).astype(jnp.int32),
        "timestep": plant(jax.random.randint(streams_of[4], (N_DP, ITEMS), 0, 1000), jax.random.fold_in(streams_of[4], 1), 0, 999).astype(jnp.int32),
        "class_id": plant(jax.random.randint(streams_of[5], (N_DP, ITEMS), 0, CLASSES), jax.random.fold_in(streams_of[5], 1), 0, CLASSES - 1).astype(jnp.int32),
        "class_table": normal_values(streams_of[6], (CLASSES, D), 1.0, 6.0),
        "ada_weight": normal_values(streams_of[7], (D, 6, D), D ** -0.5, 0.1875, ((0, 16), (2, 2)), jnp.float32),
        "ada_m": normal_values(streams_of[8], (D, 6, D), (0.0011 * TOKENS ** 0.5), 1.5, ((0, 16), (2, 2)), jnp.float32),
        "ada_v": jnp.clip(jnp.exp(math.log(0.172032) - 1.3843914 * jax.random.uniform(streams_of[9], (D, 6, D), jnp.float32) ** block_levels(streams_of[9], (D, 6, D), ((0, 16), (2, 2)), -0.2, 0.2)), 0.04308992, 0.172032),
        "ada_bias": normal_values(streams_of[10], (6, D), 0.5, 3.0, (), jnp.float32),
        "bias_m": normal_values(streams_of[11], (6, D), (0.0011 * TOKENS ** 0.5), 1.5, (), jnp.float32),
        "bias_v": jnp.clip(jnp.exp(jax.random.uniform(streams_of[12], (6, D), jnp.float32, math.log(0.04308992), math.log(0.172032))), 0.04308992, 0.172032),
        "qkv_weight": normal_values(streams_of[13], (D, 3, D), D ** -0.5, 0.1875, ((0, 16), (2, 2)), jnp.float32),
        "qkv_m": normal_values(streams_of[14], (D, 3, D), (0.0011 * TOKENS ** 0.5), 1.5, ((0, 16), (2, 2)), jnp.float32),
        "qkv_v": jnp.clip(jnp.exp(math.log(0.172032) - 1.3843914 * jax.random.uniform(streams_of[15], (D, 3, D), jnp.float32) ** block_levels(streams_of[15], (D, 3, D), ((0, 16), (2, 2)), -0.2, 0.2)), 0.04308992, 0.172032),
        "out_weight": normal_values(streams_of[16], (D, D), (D // 64) ** -0.5, 1.5, ((0, 16), (1, 2)), jnp.float32),
        "out_m": normal_values(streams_of[17], (D, D), (0.0011 * TOKENS ** 0.5), 1.5, ((0, 16), (1, 2)), jnp.float32),
        "out_v": jnp.clip(jnp.exp(math.log(0.172032) - 1.3843914 * jax.random.uniform(streams_of[18], (D, D), jnp.float32) ** block_levels(streams_of[18], (D, D), ((0, 16), (1, 2)), -0.2, 0.2)), 0.04308992, 0.172032),
        "gateup_weight": normal_values(streams_of[19], (D, 2, FF), D ** -0.5, 0.1875, ((0, 16), (2, 2)), jnp.float32),
        "gateup_m": normal_values(streams_of[20], (D, 2, FF), (0.0011 * TOKENS ** 0.5), 1.5, ((0, 16), (2, 2)), jnp.float32),
        "gateup_v": jnp.clip(jnp.exp(math.log(0.172032) - 1.3843914 * jax.random.uniform(streams_of[21], (D, 2, FF), jnp.float32) ** block_levels(streams_of[21], (D, 2, FF), ((0, 16), (2, 2)), -0.2, 0.2)), 0.04308992, 0.172032),
        "down_weight": normal_values(streams_of[22], (D, FF), FF ** -0.5, 0.109375, ((0, 16), (1, 2)), jnp.float32),
        "down_m": normal_values(streams_of[23], (D, FF), (0.0011 * TOKENS ** 0.5), 1.5, ((0, 16), (1, 2)), jnp.float32),
        "down_v": jnp.clip(jnp.exp(math.log(0.172032) - 1.3843914 * jax.random.uniform(streams_of[24], (D, FF), jnp.float32) ** block_levels(streams_of[24], (D, FF), ((0, 16), (1, 2)), -0.2, 0.2)), 0.04308992, 0.172032),
        "qk_gain": jnp.clip(1.0 + 0.15 * jax.random.normal(streams_of[25], (2, HD), jnp.float32), 0.25, 1.75),
        "gain_m": normal_values(streams_of[26], (2, HD), (0.0022 * TOKENS ** 0.5), 3.0, (), jnp.float32),
        "gain_v": jnp.clip(jnp.exp(jax.random.uniform(streams_of[27], (2, HD), jnp.float32, math.log(0.172032), math.log(0.69632))), 0.172032, 0.69632),
    }


EPSILON = 1e-06
NEG_FILL = -1e+30
PRECISE = lax.Precision.HIGHEST
BETA_FIRST = 0.9
BETA_SECOND = 0.95
ADAM_EPSILON = 1e-08
DECAY_RATE = 0.01
SMALL_RATE = 0.5

@jax.custom_vjp
def low(v):
    return lax.optimization_barrier(v.astype(jnp.bfloat16)).astype(jnp.float32)

@jax.custom_vjp
def low_back(v):
    return v

def low_keep(v):
    return (low(v), None)

def low_pass(kept, grad):
    return (grad,)

def back_keep(v):
    return (v, None)

def back_low(kept, grad):
    return (low(grad),)
low.defvjp(low_keep, low_pass)
low_back.defvjp(back_keep, back_low)

def rms_scaled(values):
    return values * lax.rsqrt(lax.optimization_barrier(jnp.mean(values * values, axis=-1, keepdims=True)) + EPSILON)

def modulate_in(base_rows, scale_rows, shift_rows):
    return rms_scaled(base_rows) * (1.0 + scale_rows) + shift_rows

def time_embed(step_ids, width):
    half_width = width // 2
    frequency = jnp.exp(-math.log(10000.0) * jnp.arange(half_width, dtype=jnp.float32) / half_width)
    angles = step_ids.astype(jnp.float32)[..., None] * frequency
    return jnp.concatenate([jnp.cos(angles), jnp.sin(angles)], axis=-1)

def layout(item_lengths, item_widths, row_index):
    ends_at = jnp.cumsum(item_lengths).astype(jnp.int32)
    starts_at = (ends_at - item_lengths).astype(jnp.int32)
    segment = lax.optimization_barrier(jnp.sum((row_index[:, None] >= ends_at[None, :]).astype(jnp.int32), axis=1)).astype(jnp.int32)
    member = segment[:, None] == jnp.arange(item_lengths.shape[0], dtype=jnp.int32)[None, :]
    offset = lax.optimization_barrier(jnp.sum(jnp.where(member, starts_at[None, :], 0), axis=1)).astype(jnp.int32)
    grid_span = lax.optimization_barrier(jnp.sum(jnp.where(member, item_widths[None, :], 0), axis=1)).astype(jnp.int32)
    inside = (row_index - offset).astype(jnp.int32)
    return (segment, (inside // grid_span).astype(jnp.int32), (inside % grid_span).astype(jnp.int32))

def rope_tables(grid_row, grid_col, head_size):
    quarter = head_size // 4
    frequency = jnp.exp(-math.log(10000.0) * jnp.arange(quarter, dtype=jnp.float32) / quarter)
    row_angle = grid_row.astype(jnp.float32)[:, None] * frequency[None, :]
    col_angle = grid_col.astype(jnp.float32)[:, None] * frequency[None, :]
    return (jnp.cos(row_angle), jnp.sin(row_angle), jnp.cos(col_angle), jnp.sin(col_angle))

def turn_half(part, cosine, sine):
    quarter = part.shape[-1] // 2
    first_part = part[..., :quarter]
    second_part = part[..., quarter:]
    cosine = cosine[:, None, :]
    sine = sine[:, None, :]
    return jnp.concatenate([first_part * cosine - second_part * sine, first_part * sine + second_part * cosine], axis=-1)

def rotate(values, tables):
    half_size = values.shape[-1] // 2
    return jnp.concatenate([turn_half(values[..., :half_size], tables[0], tables[1]), turn_half(values[..., half_size:], tables[2], tables[3])], axis=-1)

def qk_prepare(raw_query, raw_key, gains, tables):
    head_size = gains.shape[1]
    row_count = raw_query.shape[0]
    head_count = raw_query.shape[1] // head_size
    query_norm = rms_scaled(raw_query.reshape(row_count, head_count, head_size)) * gains[0]
    key_norm = rms_scaled(raw_key.reshape(row_count, head_count, head_size)) * gains[1]
    return (rotate(query_norm, tables), rotate(key_norm, tables))

def attend_ref(query_low, key_low, value_low, segment):
    block_count = GROUP_TOK // QBLOCK
    scale = HD ** (-0.5)

    def block_fn(inputs):
        queries, seg_query = inputs
        scores = jnp.einsum('qhe,khe->hqk', queries, key_low, precision=PRECISE) * scale
        scores = low_back(scores)
        allowed = (seg_query[:, None] == segment[None, :])[None]
        scores = jnp.where(allowed, scores, NEG_FILL)
        probs = low(jax.nn.softmax(scores, axis=-1))
        return jnp.einsum('hqk,khe->qhe', probs, value_low, precision=PRECISE)
    result = lax.map(jax.checkpoint(block_fn), (query_low.reshape(block_count, QBLOCK, HEADS, HD), segment.reshape(block_count, QBLOCK)))
    return result.reshape(GROUP_TOK, HEADS, HD)

def adam_update(weight, first_moment, second_moment, gradient, rate, clip):
    clipped = gradient * clip
    new_first = BETA_FIRST * first_moment + (1.0 - BETA_FIRST) * clipped
    new_second = BETA_SECOND * second_moment + (1.0 - BETA_SECOND) * clipped * clipped
    unbiased_first = new_first / (1.0 - BETA_FIRST ** STEP)
    unbiased_second = new_second / (1.0 - BETA_SECOND ** STEP)
    new_weight = weight - rate * (unbiased_first / (jnp.sqrt(unbiased_second) + ADAM_EPSILON) + DECAY_RATE * weight)
    return (new_weight, new_first, new_second)

def reference(tokens, cotangent, lengths, grid_width, timestep, class_id, class_table, ada_weight, ada_m, ada_v, ada_bias, bias_m, bias_v, qkv_weight, qkv_m, qkv_v, out_weight, out_m, out_v, gateup_weight, gateup_m, gateup_v, down_weight, down_m, down_v, qk_gain, gain_m, gain_v):
    group_count = lengths.shape[0]
    base_groups = tokens.astype(jnp.float32).reshape(group_count, GROUP_TOK, D)
    condition = class_table.astype(jnp.float32)[class_id] + time_embed(timestep, D)
    silu_cond = jax.nn.silu(condition)
    row_index = jnp.arange(GROUP_TOK, dtype=jnp.int32)
    segment, grid_row, grid_col = jax.vmap(layout, in_axes=(0, 0, None))(lengths, grid_width, row_index)
    tables = jax.vmap(partial(rope_tables, head_size=HD))(grid_row, grid_col)

    def forward(base_all, ada_w, ada_b, qkv_w, out_w, gateup_w, down_w, gains):
        ada_low = low(ada_w)
        qkv_low = low(qkv_w)
        out_low = low(out_w)
        gateup_low = low(gateup_w)
        down_low = low(down_w)
        modulation = jnp.einsum('nid,dke->nike', low(silu_cond), ada_low, precision=PRECISE) + ada_b

        def group_pass(carry, inputs):
            rows_in, mod_items, seg_rows, tabs = inputs
            mod_rows = mod_items[seg_rows]
            attn_in = low(modulate_in(rows_in, mod_rows[:, 1], mod_rows[:, 0]))
            qkv_raw = low_back(jnp.einsum('gd,dkc->kgc', attn_in, qkv_low, precision=PRECISE))
            query_rot, key_rot = qk_prepare(qkv_raw[0], qkv_raw[1], gains, tabs)
            query_low = low(query_rot)
            key_low = low(key_rot)
            value_low = low(qkv_raw[2].reshape(GROUP_TOK, HEADS, HD))
            attn_vals = attend_ref(query_low, key_low, value_low, seg_rows)
            attn_low = low(low_back(attn_vals.reshape(GROUP_TOK, D)))
            branch = low_back(jnp.einsum('gc,dc->gd', attn_low, out_low, precision=PRECISE))
            mid_rows = rows_in + mod_rows[:, 2] * branch
            mlp_in = low(modulate_in(mid_rows, mod_rows[:, 4], mod_rows[:, 3]))
            gate_up = low_back(jnp.einsum('gd,dkf->kgf', mlp_in, gateup_low, precision=PRECISE))
            hidden = low(jax.nn.silu(gate_up[0]) * gate_up[1])
            branch_mlp = low_back(jnp.einsum('gf,df->gd', hidden, down_low, precision=PRECISE))
            return (carry, mid_rows + mod_rows[:, 5] * branch_mlp)
        _, result = lax.scan(jax.checkpoint(group_pass), jnp.zeros((), jnp.float32), (base_all, modulation, segment, tables))
        return result
    block_out, pullback = jax.vjp(forward, base_groups, ada_weight, ada_bias, qkv_weight, out_weight, gateup_weight, down_weight, qk_gain)
    grads = pullback(cotangent.astype(jnp.float32).reshape(group_count, GROUP_TOK, D))
    g_input, g_ada, g_bias, g_qkv, g_out, g_gateup, g_down, g_gain = grads
    squares = jnp.sum(g_ada * g_ada) + jnp.sum(g_bias * g_bias) + jnp.sum(g_qkv * g_qkv) + jnp.sum(g_out * g_out)
    squares = squares + jnp.sum(g_gateup * g_gateup) + jnp.sum(g_down * g_down) + jnp.sum(g_gain * g_gain)
    grad_norm = jnp.sqrt(squares)
    limit = 0.01 * math.sqrt(TOKENS * PARAMS)
    clip = limit / jnp.maximum(grad_norm, limit)
    matrix_rate = D ** (-0.5)
    new_ada = adam_update(ada_weight, ada_m, ada_v, g_ada, matrix_rate, clip)
    new_bias = adam_update(ada_bias, bias_m, bias_v, g_bias, SMALL_RATE, clip)
    new_qkv = adam_update(qkv_weight, qkv_m, qkv_v, g_qkv, matrix_rate, clip)
    new_out = adam_update(out_weight, out_m, out_v, g_out, (D // 64) ** (-0.5), clip)
    new_gateup = adam_update(gateup_weight, gateup_m, gateup_v, g_gateup, matrix_rate, clip)
    new_down = adam_update(down_weight, down_m, down_v, g_down, FF ** (-0.5), clip)
    new_gain = adam_update(qk_gain, gain_m, gain_v, g_gain, SMALL_RATE, clip)
    return (block_out.reshape(TOKENS, D).astype(jnp.bfloat16), g_input.reshape(TOKENS, D).astype(jnp.bfloat16), grad_norm, new_ada[0], new_ada[1], new_ada[2], new_bias[0], new_bias[1], new_bias[2], new_qkv[0], new_qkv[1], new_qkv[2], new_out[0], new_out[1], new_out[2], new_gateup[0], new_gateup[1], new_gateup[2], new_down[0], new_down[1], new_down[2], new_gain[0], new_gain[1], new_gain[2])
```

```python
from functools import partial
import math

import jax
import jax.numpy as jnp
from jax import lax
from jax.experimental import pallas as pl
from jax.experimental.pallas import tpu as pltpu
from jax.sharding import PartitionSpec as P

D = 1152
HD = 72
FF = 3072
STEP = 10


EPSILON = 1e-06
NEG_FILL = -1e30
PRECISE = lax.Precision.HIGHEST
BETA_FIRST = 0.9
BETA_SECOND = 0.95
ADAM_EPSILON = 1e-08
DECAY_RATE = 0.01
SMALL_RATE = 0.5


def rms_scaled(values):
    return values * lax.rsqrt(jnp.mean(values * values, axis=-1, keepdims=True) + EPSILON)


def modulate_in(base_rows, scale_rows, shift_rows):
    return rms_scaled(base_rows) * (1.0 + scale_rows) + shift_rows


def time_embed(step_ids, width):
    half_width = width // 2
    frequency = jnp.exp(-math.log(10000.0) * jnp.arange(half_width, dtype=jnp.float32) / half_width)
    angles = step_ids.astype(jnp.float32)[..., None] * frequency
    return jnp.concatenate([jnp.cos(angles), jnp.sin(angles)], axis=-1)


def layout(item_lengths, item_widths, row_index):
    ends_at = jnp.cumsum(item_lengths)
    starts_at = ends_at - item_lengths
    segment = jnp.sum((row_index[:, None] >= ends_at[None, :]).astype(jnp.int32), axis=1)
    member = segment[:, None] == jnp.arange(item_lengths.shape[0], dtype=jnp.int32)[None, :]
    offset = jnp.sum(jnp.where(member, starts_at[None, :], 0), axis=1)
    grid_span = jnp.sum(jnp.where(member, item_widths[None, :], 0), axis=1)
    inside = row_index - offset
    return (segment, inside // grid_span, inside % grid_span)


def rope_tables(grid_row, grid_col, head_size):
    quarter = head_size // 4
    frequency = jnp.exp(-math.log(10000.0) * jnp.arange(quarter, dtype=jnp.float32) / quarter)
    row_angle = grid_row.astype(jnp.float32)[:, None] * frequency[None, :]
    col_angle = grid_col.astype(jnp.float32)[:, None] * frequency[None, :]
    return (jnp.cos(row_angle), jnp.sin(row_angle), jnp.cos(col_angle), jnp.sin(col_angle))


def turn_half(part, cosine, sine):
    quarter = part.shape[-1] // 2
    first_part = part[..., :quarter]
    second_part = part[..., quarter:]
    cosine = cosine[:, None, :]
    sine = sine[:, None, :]
    return jnp.concatenate(
        [first_part * cosine - second_part * sine, first_part * sine + second_part * cosine],
        axis=-1,
    )


def rotate(values, tables):
    half_size = values.shape[-1] // 2
    return jnp.concatenate(
        [
            turn_half(values[..., :half_size], tables[0], tables[1]),
            turn_half(values[..., half_size:], tables[2], tables[3]),
        ],
        axis=-1,
    )


def qk_prepare(raw_query, raw_key, gains, tables):
    head_size = gains.shape[1]
    row_count = raw_query.shape[0]
    head_count = raw_query.shape[1] // head_size
    query_norm = rms_scaled(raw_query.reshape(row_count, head_count, head_size)) * gains[0]
    key_norm = rms_scaled(raw_key.reshape(row_count, head_count, head_size)) * gains[1]
    return (rotate(query_norm, tables), rotate(key_norm, tables))


def block_geometry(total_rows):
    query_block = min(512, total_rows)
    return (query_block, total_rows, total_rows // query_block)


def window_start(block_index, query_block, key_window, total_rows):
    return jnp.clip(block_index * query_block - query_block, 0, total_rows - key_window)


def masked_scores(query_low, key_low, segment, block_index, query_block, key_window):
    total_rows = query_low.shape[0]
    scale = query_low.shape[2] ** (-0.5)
    query_start = block_index * query_block
    key_start = window_start(block_index, query_block, key_window, total_rows)
    queries = lax.dynamic_slice_in_dim(query_low, query_start, query_block, 0)
    seg_query = lax.dynamic_slice_in_dim(segment, query_start, query_block, 0)
    scores = (
        jnp.einsum("qhe,khe->hqk", queries, key_low, preferred_element_type=jnp.float32) * scale
    )
    allowed = (seg_query[:, None] == segment[None, :])[None]
    return (jnp.where(allowed, scores, NEG_FILL), queries, key_low, query_start, key_start)


def attend(query_low, key_low, value_low, segment):
    total_rows = query_low.shape[0]
    query_block, key_window, block_count = block_geometry(total_rows)

    def one_block(block_index):
        scores, queries, keyset, query_start, key_start = masked_scores(
            query_low, key_low, segment, block_index, query_block, key_window
        )
        peak = jnp.max(scores, axis=-1, keepdims=True)
        expo = jnp.exp(scores - peak)
        total_exp = jnp.sum(expo, axis=-1, keepdims=True)
        probs = (expo / total_exp).astype(jnp.bfloat16)
        result = jnp.einsum("hqk,khe->qhe", probs, value_low, preferred_element_type=jnp.float32)
        return (result, (peak + jnp.log(total_exp))[..., 0])

    outputs, log_sums = lax.map(one_block, jnp.arange(block_count, dtype=jnp.int32))
    return (outputs.reshape(total_rows, query_low.shape[1], query_low.shape[2]), log_sums)


def attend_back(query_low, key_low, value_low, d_attn, log_sums, segment):
    total_rows = query_low.shape[0]
    query_block, key_window, block_count = block_geometry(total_rows)
    scale = query_low.shape[2] ** (-0.5)
    zeros_like = jnp.zeros(query_low.shape, jnp.float32)

    def one_block(carry, block_index):
        d_keys, d_values = carry
        scores, queries, keyset, query_start, key_start = masked_scores(
            query_low, key_low, segment, block_index, query_block, key_window
        )
        grads_block = lax.dynamic_slice_in_dim(d_attn, query_start, query_block, 0)
        probs = jnp.exp(scores - log_sums[block_index][:, :, None])
        low_probs = probs.astype(jnp.bfloat16)
        d_probs = jnp.einsum(
            "qhe,khe->hqk", grads_block, value_low, preferred_element_type=jnp.float32
        )
        row_dot = jnp.sum(probs * d_probs, axis=-1, keepdims=True)
        d_scores = (probs * (d_probs - row_dot)).astype(jnp.bfloat16)
        d_query = (
            jnp.einsum("hqk,khe->qhe", d_scores, keyset, preferred_element_type=jnp.float32) * scale
        )
        d_key_part = (
            jnp.einsum("hqk,qhe->khe", d_scores, queries, preferred_element_type=jnp.float32)
            * scale
        )
        d_value_part = jnp.einsum(
            "hqk,qhe->khe", low_probs, grads_block, preferred_element_type=jnp.float32
        )
        d_keys = d_keys + d_key_part
        d_values = d_values + d_value_part
        return ((d_keys, d_values), d_query)

    (d_keys, d_values), d_queries = lax.scan(
        one_block, (zeros_like, zeros_like), jnp.arange(block_count, dtype=jnp.int32)
    )
    return (d_queries.reshape(query_low.shape), d_keys, d_values)


def adam_update(weight, first_moment, second_moment, gradient, rate, clip):
    clipped = gradient * clip
    new_first = BETA_FIRST * first_moment + (1.0 - BETA_FIRST) * clipped
    new_second = BETA_SECOND * second_moment + (1.0 - BETA_SECOND) * clipped * clipped
    unbiased_first = new_first / (1.0 - BETA_FIRST**STEP)
    unbiased_second = new_second / (1.0 - BETA_SECOND**STEP)
    new_weight = weight - rate * (
        unbiased_first / (jnp.sqrt(unbiased_second) + ADAM_EPSILON) + DECAY_RATE * weight
    )
    return (new_weight, new_first, new_second)


ZSIDE = 4
CORES = 2


def place_of(rank, count):
    xside = count // (ZSIDE * CORES)
    return (rank // (xside * CORES), (rank // CORES) % xside, rank % CORES)


def shift_pairs(count, dim, amount):
    xside = count // (ZSIDE * CORES)
    pairs = []
    for rank in range(count):
        z, x, core = place_of(rank, count)
        if dim == "z":
            z = (z + amount) % ZSIDE
        elif dim == "x":
            x = (x + amount) % xside
        else:
            core = (core + amount) % CORES
        pairs.append((rank, (z * xside + x) * CORES + core))
    return pairs


def send(values, dim, amount):
    count = lax.axis_size("dp")
    return lax.ppermute(values, "dp", shift_pairs(count, dim, amount))


def tensor_send(values, amount):
    count = lax.axis_size("tensor")
    return lax.ppermute(values, "tensor", [(r, (r + amount) % count) for r in range(count)])


def block_order(rank, count):
    xside = count // (ZSIDE * CORES)
    z, x, core = place_of(rank, count)
    flips = jnp.arange(CORES, dtype=jnp.int32)[:, None, None]
    turns = jnp.arange(xside, dtype=jnp.int32)[None, :, None]
    hops = jnp.arange(ZSIDE, dtype=jnp.int32)[None, None, :]
    their_z = (z - hops) % ZSIDE
    their_x = (x - turns) % xside
    their_core = (core + flips) % CORES
    return ((their_z * xside + their_x) * CORES + their_core).reshape(count)


def gather_pieces(shard):
    xside = lax.axis_size("dp") // (ZSIDE * CORES)
    near = jnp.concatenate([shard] + [send(shard, "z", hop) for hop in range(1, ZSIDE)], axis=0)
    mine = [near] + [send(near, "x", turn) for turn in range(1, xside)]
    other = [send(piece, "core", 1) for piece in mine]
    return mine + other


def gather_rows(shard):
    xside = lax.axis_size("dp") // (ZSIDE * CORES)
    near = jnp.concatenate([shard] + [send(shard, "z", hop) for hop in range(1, ZSIDE)], axis=0)
    mine = jnp.concatenate([near] + [send(near, "x", turn) for turn in range(1, xside)], axis=0)
    return jnp.concatenate([mine, send(mine, "core", 1)], axis=0)


def reduce_rows(mine, other):
    xside = lax.axis_size("dp") // (ZSIDE * CORES)
    kind = mine.dtype
    came = send(other, "core", 1)
    rows = mine.shape[0] // xside
    parts = []
    for turn in range(xside):
        cut = slice(turn * rows, (turn + 1) * rows)
        parts.append(mine[cut].astype(jnp.float32) + came[cut].astype(jnp.float32))
    came_x = [send(parts[turn].astype(kind), "x", -turn) for turn in range(1, xside)]
    rows = rows // ZSIDE
    cuts = []
    for hop in range(ZSIDE):
        cut = slice(hop * rows, (hop + 1) * rows)
        cuts.append(sum([piece[cut].astype(jnp.float32) for piece in came_x], parts[0][cut]))
    total = cuts[0]
    for hop in range(1, ZSIDE):
        total = total + send(cuts[hop].astype(kind), "z", -hop).astype(jnp.float32)
    return total


def tensor_gather(values):
    count = lax.axis_size("tensor")
    return jnp.concatenate([values] + [tensor_send(values, hop) for hop in range(1, count)], axis=0)


def tensor_reduce(values):
    count = lax.axis_size("tensor")
    rows = values.shape[0] // count
    total = values[:rows].astype(jnp.float32)
    for hop in range(1, count):
        came = tensor_send(values[hop * rows : (hop + 1) * rows], -hop)
        total = total + came.astype(jnp.float32)
    return total


def tensor_total(values):
    count = lax.axis_size("tensor")
    if count == 2:
        half = values.shape[0] // 2
        came = tensor_send(values, 1)
        came = jnp.concatenate([came[half:], came[:half]], axis=0)
        return values.astype(jnp.float32) + came.astype(jnp.float32)
    return tensor_gather(tensor_reduce(values).astype(values.dtype)).astype(jnp.float32)


def everywhere_sum(values):
    for axis in ("dp", "tensor"):
        count = lax.axis_size(axis)
        step = 1
        while step < count:
            values = values + lax.ppermute(values, axis, [(r, r ^ step) for r in range(count)])
            step *= 2
    return values


def mlp_kernel(pieces, has_start, rows_ref, rows_t_ref, grad_ref, grad_t_ref, *refs):
    weights = refs[:pieces]
    refs = refs[pieces:]
    if has_start:
        start_out, start_in = refs[:2]
        refs = refs[2:]
    out_ref, in_ref, mine_ref, other_ref, held, out_acc, in_acc = refs
    step = pl.program_id(0)
    share = held.shape[0] // pieces
    for index in range(pieces):
        held[index * share : (index + 1) * share, :] = weights[index][...]
    width = held.shape[1] // 3
    gate_w = held[:, :width]
    up_w = held[:, width : 2 * width]
    down_w = held[:, 2 * width :]

    @pl.when(step == 0)
    def _():
        if has_start:
            out_acc[...] = start_out[...]
            in_acc[...] = start_in[...]
        else:
            out_acc[...] = jnp.zeros_like(out_acc)
            in_acc[...] = jnp.zeros_like(in_acc)

    across = (((1,), (1,)), ((), ()))
    gate = jnp.dot(rows_ref[...], gate_w, preferred_element_type=jnp.float32)
    up = jnp.dot(rows_ref[...], up_w, preferred_element_type=jnp.float32)
    d_hidden = jnp.dot(grad_ref[...], down_w, preferred_element_type=jnp.float32)
    sigmoid = 1.0 / (1.0 + jnp.exp(-gate))
    silu = gate * sigmoid
    hidden = (silu * up).astype(jnp.bfloat16)
    d_gate = (d_hidden * up * sigmoid * (1.0 + gate * (1.0 - sigmoid))).astype(jnp.bfloat16)
    d_up = (d_hidden * silu).astype(jnp.bfloat16)
    out_acc[...] += lax.dot_general(hidden, down_w, across, preferred_element_type=jnp.float32)
    in_acc[...] += lax.dot_general(
        d_gate, gate_w, across, preferred_element_type=jnp.float32
    ) + lax.dot_general(d_up, up_w, across, preferred_element_type=jnp.float32)
    half = mine_ref.shape[0]
    for target, begin in ((mine_ref, 0), (other_ref, half)):
        rows_t = rows_t_ref[begin : begin + half, :]
        grad_t = grad_t_ref[begin : begin + half, :]
        target[:, :width] = jnp.dot(rows_t, d_gate, preferred_element_type=jnp.float32).astype(
            target.dtype
        )
        target[:, width : 2 * width] = jnp.dot(
            rows_t, d_up, preferred_element_type=jnp.float32
        ).astype(target.dtype)
        target[:, 2 * width :] = jnp.dot(
            grad_t, hidden, preferred_element_type=jnp.float32
        ).astype(target.dtype)

    @pl.when(step == pl.num_programs(0) - 1)
    def _():
        out_ref[...] = out_acc[...].astype(out_ref.dtype)
        in_ref[...] = in_acc[...].astype(in_ref.dtype)


def mlp_part(rows, rows_t, grad, grad_t, pieces, start, blocks, last):
    count, width = rows.shape
    columns = pieces[0].shape[1]
    block = columns // blocks
    whole = pl.BlockSpec((count, width), lambda i: (0, 0))
    whole_t = pl.BlockSpec((width, count), lambda i: (0, 0))
    kind = jnp.bfloat16 if last else jnp.float32
    half = jax.ShapeDtypeStruct((width // 2, columns), jnp.bfloat16)
    starts = [] if start is None else list(start)
    flops = 18 * count * width * (columns // 3)
    return pl.pallas_call(
        partial(mlp_kernel, len(pieces), len(starts) > 0),
        grid=(blocks,),
        in_specs=[whole, whole_t, whole, whole_t]
        + [pl.BlockSpec((p.shape[0], block), lambda i: (0, i)) for p in pieces]
        + [whole] * len(starts),
        out_specs=[whole, whole]
        + [pl.BlockSpec((width // 2, block), lambda i: (0, i))] * 2,
        out_shape=[jax.ShapeDtypeStruct((count, width), kind)] * 2 + [half, half],
        scratch_shapes=[
            pltpu.VMEM((width, block), jnp.bfloat16),
            pltpu.VMEM((count, width), jnp.float32),
            pltpu.VMEM((count, width), jnp.float32),
        ],
        cost_estimate=pl.CostEstimate(
            flops=flops, bytes_accessed=8 * width * columns, transcendentals=count * columns // 3
        ),
        compiler_params=pltpu.CompilerParams(vmem_limit_bytes=60 * 1024 * 1024),
    )(rows, rows_t, grad, grad_t, *pieces, *starts)


def mlp_plain(rows, grad, pieces, start, blocks, last):
    weights = jnp.concatenate(pieces, axis=0)
    width = weights.shape[0]
    block = weights.shape[1] // (3 * blocks)
    split = weights.reshape(width, blocks, 3, block)
    gate_w, up_w, down_w = [split[:, :, slot].reshape(width, blocks * block) for slot in range(3)]
    gate = jnp.dot(rows, gate_w, preferred_element_type=jnp.float32)
    up = jnp.dot(rows, up_w, preferred_element_type=jnp.float32)
    d_hidden = jnp.dot(grad, down_w, preferred_element_type=jnp.float32)
    sigmoid = jax.nn.sigmoid(gate)
    hidden = (gate * sigmoid * up).astype(jnp.bfloat16)
    d_gate = (d_hidden * up * sigmoid * (1.0 + gate * (1.0 - sigmoid))).astype(jnp.bfloat16)
    d_up = (d_hidden * gate * sigmoid).astype(jnp.bfloat16)
    out_sum = jnp.dot(hidden, down_w.T, preferred_element_type=jnp.float32)
    in_sum = jnp.dot(d_gate, gate_w.T, preferred_element_type=jnp.float32) + jnp.dot(
        d_up, up_w.T, preferred_element_type=jnp.float32
    )
    if start is not None:
        out_sum = out_sum + start[0]
        in_sum = in_sum + start[1]
    kind = jnp.bfloat16 if last else jnp.float32
    grads = [
        jnp.einsum("gd,gf->df", left, right, preferred_element_type=jnp.float32)
        .astype(jnp.bfloat16)
        .reshape(width, blocks, block)
        for left, right in ((rows, d_gate), (rows, d_up), (grad, hidden))
    ]
    packed = jnp.stack(grads, axis=2).reshape(width, 3 * blocks * block)
    return (out_sum.astype(kind), in_sum.astype(kind), packed[: width // 2], packed[width // 2 :])


def pad_columns(values, columns):
    return jnp.pad(values, ((0, 0), (0, columns - values.shape[1])))


def padded(columns):
    return -(-columns // 128) * 128


def local(
    tokens,
    cotangent,
    lengths,
    grid_width,
    timestep,
    class_id,
    class_table,
    ada_weight,
    ada_m,
    ada_v,
    ada_bias,
    bias_m,
    bias_v,
    qkv_weight,
    qkv_m,
    qkv_v,
    out_weight,
    out_m,
    out_v,
    gateup_weight,
    gateup_m,
    gateup_v,
    down_weight,
    down_m,
    down_v,
    qk_gain,
    gain_m,
    gain_v,
):
    tensor_count = lax.axis_size("tensor")
    data_count = lax.axis_size("dp")
    tensor_rank = lax.axis_index("tensor")
    data_rank = lax.axis_index("dp")
    local_rows, model_width = tokens.shape
    group_rows = local_rows * tensor_count
    column_share = model_width // tensor_count
    row_share = ada_weight.shape[0]
    head_size = qk_gain.shape[1]
    item_count = lengths.shape[1]
    class_count = class_table.shape[0]
    hidden_share = down_weight.shape[1]
    bf16 = jnp.bfloat16

    qkv_columns = padded(3 * column_share)
    out_columns = padded(column_share)
    attn_shard = jnp.concatenate(
        [
            pad_columns(qkv_weight.astype(bf16).reshape(row_share, -1), qkv_columns),
            pad_columns(out_weight.astype(bf16), out_columns),
        ],
        axis=1,
    )
    blocks = max(1, hidden_share // 512)
    block = hidden_share // (2 * blocks)
    mlp_split = jnp.stack(
        [
            part.astype(bf16).reshape(row_share, 2, blocks, block)
            for part in (gateup_weight[:, 0], gateup_weight[:, 1], down_weight)
        ],
        axis=3,
    )
    mlp_shards = [mlp_split[:, half].reshape(row_share, 3 * blocks * block) for half in range(2)]

    order = block_order(data_rank, data_count)
    column_of = (order[:, None] * row_share + jnp.arange(row_share, dtype=jnp.int32)).reshape(-1)
    to_held = (jnp.arange(model_width, dtype=jnp.int32)[:, None] == column_of[None, :]).astype(bf16)

    def hold(values):
        return jnp.dot(values, to_held, preferred_element_type=jnp.float32).astype(bf16)

    def unhold(values):
        return lax.dot_general(
            values, to_held, (((1,), (1,)), ((), ())), preferred_element_type=jnp.float32
        ).astype(bf16)

    ids = gather_rows(jnp.stack([class_id[0], timestep[0]])[None])
    item_ids = ids[:, 0].reshape(-1)
    item_steps = ids[:, 1].reshape(-1)
    class_onehot = (
        item_ids[:, None] == jnp.arange(class_count, dtype=jnp.int32)[None, :]
    ).astype(bf16)
    condition = jnp.dot(class_onehot, class_table, preferred_element_type=jnp.float32) + time_embed(
        item_steps, model_width
    )
    silu_all = jax.nn.silu(condition).astype(bf16)
    silu_own = lax.dynamic_slice_in_dim(silu_all, data_rank * row_share, row_share, 1)
    mod_part = jnp.dot(
        silu_own,
        ada_weight.astype(bf16).reshape(row_share, 6 * column_share),
        preferred_element_type=jnp.float32,
    )
    half_items = data_count * item_count // 2
    mod_share = reduce_rows(mod_part[:half_items], mod_part[half_items:])
    bias_share = lax.dynamic_slice_in_dim(ada_bias, tensor_rank * column_share, column_share, 1)
    mod_share = mod_share.reshape(item_count, 6, column_share) + bias_share[None]
    if tensor_count == 2:
        mod_other = tensor_send(mod_share, 1)
        lower = jnp.where(tensor_rank == 0, mod_share, mod_other)
        upper = jnp.where(tensor_rank == 0, mod_other, mod_share)
        modulation = jnp.concatenate([lower, upper], axis=2)
    else:
        modulation = lax.all_gather(mod_share, "tensor", axis=2, tiled=True)
    modulation = jnp.dot(
        modulation.reshape(item_count * 6, model_width),
        to_held.astype(jnp.float32),
        precision=PRECISE,
        preferred_element_type=jnp.float32,
    ).reshape(item_count, 6, model_width)

    tokens_all = hold(tensor_gather(tokens))
    cot_all = hold(tensor_gather(cotangent))
    base_rows = tokens_all.astype(jnp.float32)
    cot_rows = cot_all.astype(jnp.float32)
    row_blocks = (tensor_rank - jnp.arange(tensor_count, dtype=jnp.int32)) % tensor_count
    row_index = (
        row_blocks[:, None] * local_rows + jnp.arange(local_rows, dtype=jnp.int32)[None, :]
    ).reshape(-1)
    segment, grid_row, grid_col = layout(lengths[0], grid_width[0], row_index)
    tables = rope_tables(grid_row, grid_col, head_size)

    def mod_rows(slot, count):
        picked = modulation[0, slot][None, :]
        for item in range(1, item_count):
            picked = jnp.where(
                segment[:count, None] == item, modulation[item, slot][None, :], picked
            )
        return picked

    def mod_sums(values):
        own = segment[:local_rows]
        return jnp.stack(
            [
                jnp.sum(jnp.where(own[:, None] == item, values, 0.0), axis=0)
                for item in range(item_count)
            ]
        )

    attn_pieces = gather_pieces(attn_shard)
    mlp_pieces = [gather_pieces(shard) for shard in mlp_shards]
    attn_full = jnp.concatenate(attn_pieces, axis=0)
    full_qkv = attn_full[:, : 3 * column_share]
    full_out = attn_full[:, qkv_columns : qkv_columns + column_share]

    attn_in = modulate_in(base_rows, mod_rows(1, group_rows), mod_rows(0, group_rows)).astype(bf16)
    qkv_raw = jnp.dot(attn_in, full_qkv, preferred_element_type=jnp.float32)
    raw_query, raw_key, raw_value = [
        qkv_raw[:, slot * column_share : (slot + 1) * column_share] for slot in range(3)
    ]
    query_rot, key_rot = qk_prepare(raw_query, raw_key, qk_gain, tables)
    query_low = query_rot.astype(bf16)
    key_low = key_rot.astype(bf16)
    value_low = raw_value.reshape(group_rows, -1, head_size).astype(bf16)
    attn_vals, log_sums = attend(query_low, key_low, value_low, segment)
    attn_low = attn_vals.reshape(group_rows, column_share).astype(bf16)
    branch = tensor_total(
        jnp.einsum("gc,dc->gd", attn_low, full_out, preferred_element_type=jnp.float32).astype(bf16)
    )
    mid_rows = base_rows + mod_rows(2, group_rows) * branch
    scale_two = mod_rows(4, group_rows)
    mlp_in = modulate_in(mid_rows, scale_two, mod_rows(3, group_rows)).astype(bf16)
    gate_two = mod_rows(5, group_rows)
    d_branch_mlp = (gate_two * cot_rows).astype(bf16)

    if group_rows <= 512:
        mlp_in_t = mlp_in.T
        d_branch_t = d_branch_mlp.T
        first = mlp_part(
            mlp_in, mlp_in_t, d_branch_mlp, d_branch_t, mlp_pieces[0], None, blocks, False
        )
        second = mlp_part(
            mlp_in, mlp_in_t, d_branch_mlp, d_branch_t, mlp_pieces[1], first[:2], blocks, True
        )
    else:
        first = mlp_plain(mlp_in, d_branch_mlp, mlp_pieces[0], None, blocks, False)
        second = mlp_plain(mlp_in, d_branch_mlp, mlp_pieces[1], first[:2], blocks, True)
    d_mlp_in = tensor_total(second[1])
    branch_mlp = tensor_reduce(second[0])
    out_rows = mid_rows[:local_rows] + gate_two[:local_rows] * branch_mlp
    out_tokens = unhold(out_rows.astype(bf16))
    sum_mlp = [reduce_rows(part[2], part[3]) for part in (first, second)]

    d_mid_norm, d_scale_two, d_shift_two = jax.vjp(
        modulate_in, mid_rows, scale_two, jnp.zeros_like(mid_rows)
    )[1](d_mlp_in)
    d_mid = cot_rows + d_mid_norm
    d_branch_attn = (mod_rows(2, group_rows) * d_mid).astype(bf16)
    half_width = model_width // 2
    g_out = [
        jnp.einsum("gd,gc->dc", part, attn_low, preferred_element_type=jnp.float32).astype(bf16)
        for part in (d_branch_attn[:, :half_width], d_branch_attn[:, half_width:])
    ]
    sum_out = reduce_rows(g_out[0], g_out[1])
    d_attn = jnp.einsum("gd,dc->gc", d_branch_attn, full_out, preferred_element_type=jnp.float32)
    d_attn = d_attn.astype(bf16).reshape(query_low.shape)
    d_query_rot, d_key_rot, d_values = attend_back(
        query_low, key_low, value_low, d_attn, log_sums, segment
    )
    _, pull_qk = jax.vjp(partial(qk_prepare, tables=tables), raw_query, raw_key, qk_gain)
    d_query_raw, d_key_raw, g_gain = pull_qk((d_query_rot, d_key_rot))
    d_qkv_low = jnp.concatenate(
        [d_query_raw, d_key_raw, d_values.reshape(group_rows, column_share)], axis=1
    ).astype(bf16)
    d_attn_part = jnp.einsum("gc,dc->gd", d_qkv_low, full_qkv, preferred_element_type=jnp.float32)
    d_attn_in = tensor_reduce(d_attn_part.astype(bf16))
    g_qkv = [
        jnp.einsum("gd,gc->dc", part, d_qkv_low, preferred_element_type=jnp.float32).astype(bf16)
        for part in (attn_in[:, :half_width], attn_in[:, half_width:])
    ]
    sum_qkv = reduce_rows(g_qkv[0], g_qkv[1])

    own_scale = mod_rows(1, local_rows)
    d_base_norm, d_scale_one, d_shift_one = jax.vjp(
        modulate_in, base_rows[:local_rows], own_scale, jnp.zeros_like(own_scale)
    )[1](d_attn_in)
    input_grad = unhold((d_mid[:local_rows] + d_base_norm).astype(bf16))
    d_mod_part = jnp.stack(
        [
            mod_sums(d_shift_one),
            mod_sums(d_scale_one),
            mod_sums(d_mid[:local_rows] * branch[:local_rows]),
            mod_sums(d_shift_two[:local_rows]),
            mod_sums(d_scale_two[:local_rows]),
            mod_sums(cot_rows[:local_rows] * branch_mlp),
        ],
        axis=1,
    )
    d_mod_part = lax.dot_general(
        d_mod_part.reshape(item_count * 6, model_width),
        to_held.astype(jnp.float32),
        (((1,), (1,)), ((), ())),
        precision=PRECISE,
        preferred_element_type=jnp.float32,
    ).reshape(item_count, 6, model_width)
    if tensor_count == 2:
        lower, upper = d_mod_part[:, :, :column_share], d_mod_part[:, :, column_share:]
        theirs = jnp.where(tensor_rank == 0, upper, lower)
        d_mod = jnp.where(tensor_rank == 0, lower, upper) + tensor_send(theirs, 1)
    else:
        d_mod = lax.psum_scatter(d_mod_part, "tensor", scatter_dimension=2, tiled=True)
    d_mod_all = gather_rows(d_mod.reshape(item_count, 6 * column_share))
    sum_ada = lax.dot_general(
        silu_own.astype(jnp.float32),
        d_mod_all,
        (((0,), (0,)), ((), ())),
        precision=PRECISE,
        preferred_element_type=jnp.float32,
    )
    bias_share = jnp.sum(d_mod_all, axis=0).reshape(6, column_share)
    if tensor_count == 2:
        bias_other = tensor_send(bias_share, 1)
        lower = jnp.where(tensor_rank == 0, bias_share, bias_other)
        upper = jnp.where(tensor_rank == 0, bias_other, bias_share)
        bias_grad = jnp.concatenate([lower, upper], axis=1)
    else:
        bias_grad = lax.all_gather(bias_share, "tensor", axis=1, tiled=True)

    local_squares = jnp.sum(sum_ada * sum_ada) + jnp.sum(sum_qkv * sum_qkv)
    local_squares = local_squares + jnp.sum(sum_out * sum_out)
    for part in sum_mlp:
        local_squares = local_squares + jnp.sum(part * part)
    packet = jnp.concatenate(
        [
            g_gain.reshape(-1),
            local_squares[None],
            jnp.zeros((256 - 2 * head_size - 1,), jnp.float32),
        ]
    ).reshape(2, 128)
    packet = everywhere_sum(packet).reshape(-1)
    gain_total = packet[: 2 * head_size].reshape(2, head_size)
    grad_norm = jnp.sqrt(
        packet[2 * head_size] + jnp.sum(gain_total * gain_total) + jnp.sum(bias_grad * bias_grad)
    )
    tokens_all_count = local_rows * tensor_count * data_count
    params_all = 10 * D * D + 3 * D * FF + 6 * D + 2 * HD
    limit = 0.01 * math.sqrt(tokens_all_count * params_all)
    clip = limit / jnp.maximum(grad_norm, limit)
    matrix_rate = model_width ** (-0.5)

    g_ada = sum_ada.reshape(ada_weight.shape)
    g_qkv_sum = sum_qkv.reshape(qkv_weight.shape)
    mlp_sum = jnp.stack(
        [part.reshape(row_share, blocks, 3, block) for part in sum_mlp], axis=1
    )
    g_gateup = jnp.stack(
        [mlp_sum[:, :, :, slot].reshape(row_share, hidden_share) for slot in range(2)], axis=1
    )
    g_down = mlp_sum[:, :, :, 2].reshape(row_share, hidden_share)

    new_ada = adam_update(ada_weight, ada_m, ada_v, g_ada, matrix_rate, clip)
    new_bias = adam_update(ada_bias, bias_m, bias_v, bias_grad, SMALL_RATE, clip)
    new_qkv = adam_update(qkv_weight, qkv_m, qkv_v, g_qkv_sum, matrix_rate, clip)
    new_out = adam_update(out_weight, out_m, out_v, sum_out, (model_width // 64) ** (-0.5), clip)
    new_gateup = adam_update(gateup_weight, gateup_m, gateup_v, g_gateup, matrix_rate, clip)
    new_down = adam_update(down_weight, down_m, down_v, g_down, FF ** (-0.5), clip)
    new_gain = adam_update(qk_gain, gain_m, gain_v, gain_total, SMALL_RATE, clip)
    return (
        out_tokens,
        input_grad,
        grad_norm,
        new_ada[0],
        new_ada[1],
        new_ada[2],
        new_bias[0],
        new_bias[1],
        new_bias[2],
        new_qkv[0],
        new_qkv[1],
        new_qkv[2],
        new_out[0],
        new_out[1],
        new_out[2],
        new_gateup[0],
        new_gateup[1],
        new_gateup[2],
        new_down[0],
        new_down[1],
        new_down[2],
        new_gain[0],
        new_gain[1],
        new_gain[2],
    )


def solution(mesh):
    in_specs = (
        P(("dp", "tensor"), None),
        P(("dp", "tensor"), None),
        P("dp", None),
        P("dp", None),
        P("dp", None),
        P("dp", None),
        P(),
        P("dp", None, "tensor"),
        P("dp", None, "tensor"),
        P("dp", None, "tensor"),
        P(),
        P(),
        P(),
        P("dp", None, "tensor"),
        P("dp", None, "tensor"),
        P("dp", None, "tensor"),
        P("dp", "tensor"),
        P("dp", "tensor"),
        P("dp", "tensor"),
        P("dp", None, "tensor"),
        P("dp", None, "tensor"),
        P("dp", None, "tensor"),
        P("dp", "tensor"),
        P("dp", "tensor"),
        P("dp", "tensor"),
        P(),
        P(),
        P(),
    )
    out_specs = (
        P(("dp", "tensor"), None),
        P(("dp", "tensor"), None),
        P(),
        P("dp", None, "tensor"),
        P("dp", None, "tensor"),
        P("dp", None, "tensor"),
        P(),
        P(),
        P(),
        P("dp", None, "tensor"),
        P("dp", None, "tensor"),
        P("dp", None, "tensor"),
        P("dp", "tensor"),
        P("dp", "tensor"),
        P("dp", "tensor"),
        P("dp", None, "tensor"),
        P("dp", None, "tensor"),
        P("dp", None, "tensor"),
        P("dp", "tensor"),
        P("dp", "tensor"),
        P("dp", "tensor"),
        P(),
        P(),
        P(),
    )
    return jax.shard_map(local, mesh=mesh, in_specs=in_specs, out_specs=out_specs, check_vma=False)
```

```python
from functools import partial
import math

import jax
import jax.numpy as jnp
from jax import lax
from jax.experimental import pallas as pl
from jax.experimental.layout import Layout, with_layout_constraint
from jax.experimental.pallas import tpu as pltpu
from jax.sharding import PartitionSpec as P

D = 1152
HD = 72
FF = 3072
STEP = 10


EPSILON = 1e-06
NEG_FILL = -1e30
PRECISE = lax.Precision.HIGHEST
BETA_FIRST = 0.9
BETA_SECOND = 0.95
ADAM_EPSILON = 1e-08
DECAY_RATE = 0.01
SMALL_RATE = 0.5


def rms_scaled(values):
    return values * lax.rsqrt(jnp.mean(values * values, axis=-1, keepdims=True) + EPSILON)


def modulate_in(base_rows, scale_rows, shift_rows):
    return rms_scaled(base_rows) * (1.0 + scale_rows) + shift_rows


def time_embed(step_ids, width):
    half_width = width // 2
    frequency = jnp.exp(-math.log(10000.0) * jnp.arange(half_width, dtype=jnp.float32) / half_width)
    angles = step_ids.astype(jnp.float32)[..., None] * frequency
    return jnp.concatenate([jnp.cos(angles), jnp.sin(angles)], axis=-1)


def layout(item_lengths, item_widths, row_index):
    ends_at = jnp.cumsum(item_lengths)
    starts_at = ends_at - item_lengths
    segment = jnp.sum((row_index[:, None] >= ends_at[None, :]).astype(jnp.int32), axis=1)
    member = segment[:, None] == jnp.arange(item_lengths.shape[0], dtype=jnp.int32)[None, :]
    offset = jnp.sum(jnp.where(member, starts_at[None, :], 0), axis=1)
    grid_span = jnp.sum(jnp.where(member, item_widths[None, :], 0), axis=1)
    inside = row_index - offset
    return (segment, inside // grid_span, inside % grid_span)


def rope_tables(grid_row, grid_col, head_size):
    quarter = head_size // 4
    frequency = jnp.exp(-math.log(10000.0) * jnp.arange(quarter, dtype=jnp.float32) / quarter)
    row_angle = grid_row.astype(jnp.float32)[:, None] * frequency[None, :]
    col_angle = grid_col.astype(jnp.float32)[:, None] * frequency[None, :]
    return (jnp.cos(row_angle), jnp.sin(row_angle), jnp.cos(col_angle), jnp.sin(col_angle))


def turn_half(part, cosine, sine):
    quarter = part.shape[-1] // 2
    first_part = part[..., :quarter]
    second_part = part[..., quarter:]
    cosine = cosine[:, None, :]
    sine = sine[:, None, :]
    return jnp.concatenate(
        [first_part * cosine - second_part * sine, first_part * sine + second_part * cosine],
        axis=-1,
    )


def rotate(values, tables):
    half_size = values.shape[-1] // 2
    return jnp.concatenate(
        [
            turn_half(values[..., :half_size], tables[0], tables[1]),
            turn_half(values[..., half_size:], tables[2], tables[3]),
        ],
        axis=-1,
    )


def qk_prepare(raw_query, raw_key, gains, tables):
    head_size = gains.shape[1]
    row_count = raw_query.shape[0]
    head_count = raw_query.shape[1] // head_size
    query_norm = rms_scaled(raw_query.reshape(row_count, head_count, head_size)) * gains[0]
    key_norm = rms_scaled(raw_key.reshape(row_count, head_count, head_size)) * gains[1]
    return (rotate(query_norm, tables), rotate(key_norm, tables))


def block_geometry(total_rows):
    query_block = min(512, total_rows)
    return (query_block, total_rows, total_rows // query_block)


def window_start(block_index, query_block, key_window, total_rows):
    return jnp.clip(block_index * query_block - query_block, 0, total_rows - key_window)


def masked_scores(query_low, key_low, segment, block_index, query_block, key_window):
    total_rows = query_low.shape[0]
    scale = query_low.shape[2] ** (-0.5)
    query_start = block_index * query_block
    key_start = window_start(block_index, query_block, key_window, total_rows)
    queries = lax.dynamic_slice_in_dim(query_low, query_start, query_block, 0)
    seg_query = lax.dynamic_slice_in_dim(segment, query_start, query_block, 0)
    scores = (
        jnp.einsum("qhe,khe->hqk", queries, key_low, preferred_element_type=jnp.float32) * scale
    )
    allowed = (seg_query[:, None] == segment[None, :])[None]
    return (jnp.where(allowed, scores, NEG_FILL), queries, key_low, query_start, key_start)


def attend(query_low, key_low, value_low, segment):
    total_rows = query_low.shape[0]
    query_block, key_window, block_count = block_geometry(total_rows)

    def one_block(block_index):
        scores, queries, keyset, query_start, key_start = masked_scores(
            query_low, key_low, segment, block_index, query_block, key_window
        )
        peak = jnp.max(scores, axis=-1, keepdims=True)
        expo = jnp.exp(scores - peak)
        total_exp = jnp.sum(expo, axis=-1, keepdims=True)
        probs = (expo / total_exp).astype(jnp.bfloat16)
        result = jnp.einsum("hqk,khe->qhe", probs, value_low, preferred_element_type=jnp.float32)
        return (result, (peak + jnp.log(total_exp))[..., 0])

    outputs, log_sums = lax.map(one_block, jnp.arange(block_count, dtype=jnp.int32))
    return (outputs.reshape(total_rows, query_low.shape[1], query_low.shape[2]), log_sums)


def attend_back(query_low, key_low, value_low, d_attn, log_sums, segment):
    total_rows = query_low.shape[0]
    query_block, key_window, block_count = block_geometry(total_rows)
    scale = query_low.shape[2] ** (-0.5)
    zeros_like = jnp.zeros(query_low.shape, jnp.float32)

    def one_block(carry, block_index):
        d_keys, d_values = carry
        scores, queries, keyset, query_start, key_start = masked_scores(
            query_low, key_low, segment, block_index, query_block, key_window
        )
        grads_block = lax.dynamic_slice_in_dim(d_attn, query_start, query_block, 0)
        probs = jnp.exp(scores - log_sums[block_index][:, :, None])
        low_probs = probs.astype(jnp.bfloat16)
        d_probs = jnp.einsum(
            "qhe,khe->hqk", grads_block, value_low, preferred_element_type=jnp.float32
        )
        row_dot = jnp.sum(probs * d_probs, axis=-1, keepdims=True)
        d_scores = (probs * (d_probs - row_dot)).astype(jnp.bfloat16)
        d_query = (
            jnp.einsum("hqk,khe->qhe", d_scores, keyset, preferred_element_type=jnp.float32) * scale
        )
        d_key_part = (
            jnp.einsum("hqk,qhe->khe", d_scores, queries, preferred_element_type=jnp.float32)
            * scale
        )
        d_value_part = jnp.einsum(
            "hqk,qhe->khe", low_probs, grads_block, preferred_element_type=jnp.float32
        )
        d_keys = d_keys + d_key_part
        d_values = d_values + d_value_part
        return ((d_keys, d_values), d_query)

    (d_keys, d_values), d_queries = lax.scan(
        one_block, (zeros_like, zeros_like), jnp.arange(block_count, dtype=jnp.int32)
    )
    return (d_queries.reshape(query_low.shape), d_keys, d_values)


def adam_update(weight, first_moment, second_moment, gradient, rate, clip):
    clipped = gradient * clip
    new_first = BETA_FIRST * first_moment + (1.0 - BETA_FIRST) * clipped
    new_second = BETA_SECOND * second_moment + (1.0 - BETA_SECOND) * clipped * clipped
    unbiased_first = new_first / (1.0 - BETA_FIRST**STEP)
    unbiased_second = new_second / (1.0 - BETA_SECOND**STEP)
    new_weight = weight - rate * (
        unbiased_first / (jnp.sqrt(unbiased_second) + ADAM_EPSILON) + DECAY_RATE * weight
    )
    return (new_weight, new_first, new_second)


ZSIDE = 4
CORES = 2


def place_of(rank, count):
    xside = count // (ZSIDE * CORES)
    return (rank // (xside * CORES), (rank // CORES) % xside, rank % CORES)


def shift_pairs(count, dim, amount):
    xside = count // (ZSIDE * CORES)
    pairs = []
    for rank in range(count):
        z, x, core = place_of(rank, count)
        if dim == "z":
            z = (z + amount) % ZSIDE
        elif dim == "x":
            x = (x + amount) % xside
        else:
            core = (core + amount) % CORES
        pairs.append((rank, (z * xside + x) * CORES + core))
    return pairs


def send(values, dim, amount):
    count = lax.axis_size("dp")
    return lax.ppermute(values, "dp", shift_pairs(count, dim, amount))


def tensor_send(values, amount):
    count = lax.axis_size("tensor")
    return lax.ppermute(values, "tensor", [(r, (r + amount) % count) for r in range(count)])


def block_order(rank, count):
    xside = count // (ZSIDE * CORES)
    z, x, core = place_of(rank, count)
    flips = jnp.arange(CORES, dtype=jnp.int32)[:, None, None]
    turns = jnp.arange(xside, dtype=jnp.int32)[None, :, None]
    hops = jnp.arange(ZSIDE, dtype=jnp.int32)[None, None, :]
    their_z = (z - hops) % ZSIDE
    their_x = (x - turns) % xside
    their_core = (core + flips) % CORES
    return ((their_z * xside + their_x) * CORES + their_core).reshape(count)


def gather_rows(shard):
    xside = lax.axis_size("dp") // (ZSIDE * CORES)
    near = jnp.concatenate([shard] + [send(shard, "z", hop) for hop in range(1, ZSIDE)], axis=0)
    mine = jnp.concatenate([near] + [send(near, "x", turn) for turn in range(1, xside)], axis=0)
    return jnp.concatenate([mine, send(mine, "core", 1)], axis=0)


def by_rows(values):
    return with_layout_constraint(values, Layout(tuple(range(values.ndim))))


def gated(value, gate):
    return lax.optimization_barrier((value, gate))


def fold_core(mine, other):
    xside = lax.axis_size("dp") // (ZSIDE * CORES)
    came = send(other, "core", 1)
    rows = mine.shape[0] // xside
    parts = []
    for turn in range(xside):
        cut = slice(turn * rows, (turn + 1) * rows)
        added = mine[cut].astype(jnp.float32) + came[cut].astype(jnp.float32)
        parts.append(added.astype(mine.dtype))
    return parts


def fold_x(parts):
    came = [send(parts[turn], "x", -turn) for turn in range(1, len(parts))]
    rows = parts[0].shape[0] // ZSIDE
    cuts = []
    for hop in range(ZSIDE):
        cut = slice(hop * rows, (hop + 1) * rows)
        added = parts[0][cut].astype(jnp.float32)
        for piece in came:
            added = added + piece[cut].astype(jnp.float32)
        cuts.append(added.astype(parts[0].dtype))
    return cuts


def fold_z(cuts):
    total = cuts[0].astype(jnp.float32)
    for hop in range(1, ZSIDE):
        total = total + send(cuts[hop], "z", -hop).astype(jnp.float32)
    return total


def reduce_rows(mine, other):
    return fold_z(fold_x(fold_core(mine, other)))


def split_core(gradient):
    count = lax.axis_size("dp")
    xside = count // (ZSIDE * CORES)
    z, x, core = place_of(lax.axis_index("dp"), count)
    rows = gradient.shape[0] // count
    blocks = gradient.reshape(ZSIDE, xside, CORES, rows, -1)
    halves = []
    for side in (core, 1 - core):
        half = lax.dynamic_index_in_dim(blocks, side, 2, keepdims=False)
        turns = [(x - turn) % xside for turn in range(xside)]
        cut = [lax.dynamic_index_in_dim(half, turn, 1, keepdims=False) for turn in turns]
        halves.append(cut)
    return halves


def fold_rows(gradient):
    z = place_of(lax.axis_index("dp"), lax.axis_size("dp"))[0]
    kind = gradient.dtype
    mine, other = split_core(gradient)
    parts = []
    for own, theirs in zip(mine, other):
        came = send(theirs, "core", 1)
        parts.append((own.astype(jnp.float32) + came.astype(jnp.float32)).astype(kind))
    total = parts[0].astype(jnp.float32)
    for turn in range(1, len(parts)):
        total = total + send(parts[turn], "x", -turn).astype(jnp.float32)
    cuts = [
        lax.dynamic_index_in_dim(total, (z - hop) % ZSIDE, 0, keepdims=False) for hop in range(ZSIDE)
    ]
    total = cuts[0]
    for hop in range(1, ZSIDE):
        total = total + send(cuts[hop].astype(kind), "z", -hop).astype(jnp.float32)
    return total


def tensor_gather(values):
    count = lax.axis_size("tensor")
    return jnp.concatenate([values] + [tensor_send(values, hop) for hop in range(1, count)], axis=0)


def tensor_reduce(values):
    count = lax.axis_size("tensor")
    rows = values.shape[0] // count
    total = values[:rows].astype(jnp.float32)
    for hop in range(1, count):
        came = tensor_send(values[hop * rows : (hop + 1) * rows], -hop)
        total = total + came.astype(jnp.float32)
    return total


def tensor_total(values):
    count = lax.axis_size("tensor")
    if count == 2:
        half = values.shape[0] // 2
        came = tensor_send(values, 1)
        came = jnp.concatenate([came[half:], came[:half]], axis=0)
        return values.astype(jnp.float32) + came.astype(jnp.float32)
    return tensor_gather(tensor_reduce(values).astype(values.dtype)).astype(jnp.float32)


def everywhere_sum(values):
    for axis in ("dp", "tensor"):
        count = lax.axis_size(axis)
        step = 1
        while step < count:
            values = values + lax.ppermute(values, axis, [(r, r ^ step) for r in range(count)])
            step *= 2
    return values


def mlp_kernel(rows_ref, rows_t_ref, grad_ref, grad_t_ref, held, *refs):
    out_ref, in_ref, target, out_acc, in_acc = refs
    step = pl.program_id(0)
    width = held.shape[1] // 3
    gate_w = held[:, :width]
    up_w = held[:, width : 2 * width]
    down_w = held[:, 2 * width :]

    @pl.when(step == 0)
    def _():
        out_acc[...] = jnp.zeros_like(out_acc)
        in_acc[...] = jnp.zeros_like(in_acc)

    across = (((1,), (1,)), ((), ()))
    gate = jnp.dot(rows_ref[...], gate_w, preferred_element_type=jnp.float32)
    up = jnp.dot(rows_ref[...], up_w, preferred_element_type=jnp.float32)
    d_hidden = jnp.dot(grad_ref[...], down_w, preferred_element_type=jnp.float32)
    sigmoid = 1.0 / (1.0 + jnp.exp(-gate))
    silu = gate * sigmoid
    hidden = (silu * up).astype(jnp.bfloat16)
    d_gate = (d_hidden * up * sigmoid * (1.0 + gate * (1.0 - sigmoid))).astype(jnp.bfloat16)
    d_up = (d_hidden * silu).astype(jnp.bfloat16)
    out_acc[...] += lax.dot_general(hidden, down_w, across, preferred_element_type=jnp.float32)
    in_acc[...] += lax.dot_general(
        d_gate, gate_w, across, preferred_element_type=jnp.float32
    ) + lax.dot_general(d_up, up_w, across, preferred_element_type=jnp.float32)
    rows_t = rows_t_ref[...]
    for at, left, right in (
        (0, rows_t, d_gate),
        (width, rows_t, d_up),
        (2 * width, grad_t_ref[...], hidden),
    ):
        product = jnp.dot(left, right, preferred_element_type=jnp.float32)
        target[:, at : at + width] = product.astype(target.dtype)

    @pl.when(step == pl.num_programs(0) - 1)
    def _():
        out_ref[...] = out_acc[...].astype(out_ref.dtype)
        in_ref[...] = in_acc[...].astype(in_ref.dtype)


def mlp_part(rows, grad, weights, blocks):
    count, width = rows.shape
    columns = weights.shape[1]
    block = columns // blocks
    whole = pl.BlockSpec((count, width), lambda i: (0, 0))
    whole_t = pl.BlockSpec((width, count), lambda i: (0, 0))
    across = pl.BlockSpec((width, block), lambda i: (0, i))
    return pl.pallas_call(
        mlp_kernel,
        grid=(blocks,),
        in_specs=[whole, whole_t, whole, whole_t, across],
        out_specs=[whole, whole, across],
        out_shape=[jax.ShapeDtypeStruct((count, width), jnp.bfloat16)] * 2
        + [jax.ShapeDtypeStruct((width, columns), jnp.bfloat16)],
        scratch_shapes=[pltpu.VMEM((count, width), jnp.float32)] * 2,
        cost_estimate=pl.CostEstimate(
            flops=6 * count * width * columns,
            bytes_accessed=4 * width * columns,
            transcendentals=count * columns // 3,
        ),
        compiler_params=pltpu.CompilerParams(vmem_limit_bytes=60 * 1024 * 1024),
    )(rows, rows.T, grad, grad.T, weights)


def mlp_plain(rows, grad, weights, blocks):
    width = weights.shape[0]
    block = weights.shape[1] // (3 * blocks)
    split = weights.reshape(width, blocks, 3, block)
    gate_w, up_w, down_w = [split[:, :, slot].reshape(width, blocks * block) for slot in range(3)]
    gate = jnp.dot(rows, gate_w, preferred_element_type=jnp.float32)
    up = jnp.dot(rows, up_w, preferred_element_type=jnp.float32)
    d_hidden = jnp.dot(grad, down_w, preferred_element_type=jnp.float32)
    sigmoid = jax.nn.sigmoid(gate)
    hidden = (gate * sigmoid * up).astype(jnp.bfloat16)
    d_gate = (d_hidden * up * sigmoid * (1.0 + gate * (1.0 - sigmoid))).astype(jnp.bfloat16)
    d_up = (d_hidden * gate * sigmoid).astype(jnp.bfloat16)
    out_sum = jnp.dot(hidden, down_w.T, preferred_element_type=jnp.float32)
    in_sum = jnp.dot(d_gate, gate_w.T, preferred_element_type=jnp.float32) + jnp.dot(
        d_up, up_w.T, preferred_element_type=jnp.float32
    )
    grads = [
        jnp.einsum("gd,gf->df", left, right, preferred_element_type=jnp.float32)
        .astype(jnp.bfloat16)
        .reshape(width, blocks, block)
        for left, right in ((rows, d_gate), (rows, d_up), (grad, hidden))
    ]
    packed = jnp.stack(grads, axis=2).reshape(width, 3 * blocks * block)
    return (out_sum.astype(jnp.bfloat16), in_sum.astype(jnp.bfloat16), packed)


def pack_kernel(stride, block, qkv_ref, out_ref, gateup_ref, down_ref, attn_low, mlp_low):
    columns = out_ref.shape[1]
    attn_low[...] = jnp.zeros_like(attn_low)
    for slot in range(3):
        attn_low[:, slot * stride : slot * stride + columns] = qkv_ref[slot].astype(jnp.bfloat16)
    attn_low[:, 3 * stride : 3 * stride + columns] = out_ref[...].astype(jnp.bfloat16)
    for begin in range(0, down_ref.shape[1], block):
        cut = slice(begin, begin + block)
        at = 3 * begin
        mlp_low[:, at : at + block] = gateup_ref[0, :, cut].astype(jnp.bfloat16)
        mlp_low[:, at + block : at + 2 * block] = gateup_ref[1, :, cut].astype(jnp.bfloat16)
        mlp_low[:, at + 2 * block : at + 3 * block] = down_ref[:, cut].astype(jnp.bfloat16)


def pack(qkv, out, gateup, down, stride, block):
    rows, hidden = down.shape
    low = lambda columns: jax.ShapeDtypeStruct((rows, columns), jnp.bfloat16)
    return pl.pallas_call(
        partial(pack_kernel, stride, block), out_shape=[low(4 * stride), low(3 * hidden)]
    )(qkv, out, gateup, down)


def mod_kernel(stride, rows_ref, ada_ref, target):
    columns = ada_ref.shape[2]
    target[...] = jnp.zeros_like(target)
    for slot in range(ada_ref.shape[0]):
        target[:, slot * stride : slot * stride + columns] = jnp.dot(
            rows_ref[...], ada_ref[slot].astype(jnp.bfloat16), preferred_element_type=jnp.float32
        )


def mod_product(rows, ada, stride):
    return pl.pallas_call(
        partial(mod_kernel, stride),
        out_shape=jax.ShapeDtypeStruct((rows.shape[0], ada.shape[0] * stride), jnp.float32),
    )(rows, ada)


def adam_kernel(stride, block, rates, clip_ref, *refs):
    clip = clip_ref[0, 0]
    ada_g, qkv_g, out_g, mlp_g, bias_g, gain_g = refs[:6]
    states, targets = refs[6:27], refs[27:]
    ada, bias, qkv, out, gateup, down, gain = [
        (states[3 * i : 3 * i + 3], targets[3 * i : 3 * i + 3], rates[i]) for i in range(7)
    ]

    def step(group, index, gradient):
        held, put, rate = group
        result = adam_update(*[ref[index] for ref in held], gradient, rate, clip)
        for ref, value in zip(put, result):
            ref[index] = value

    columns = out[0][0].shape[1]
    for group, source in ((ada, ada_g), (qkv, qkv_g)):
        for slot in range(group[0][0].shape[0]):
            step(group, slot, source[:, slot * stride : slot * stride + columns])
    step(out, slice(None), out_g[:, :columns])
    for begin in range(0, down[0][0].shape[1], block):
        cut = slice(begin, begin + block)
        at = 3 * begin
        for slot, group, index in (
            (0, gateup, (0, slice(None), cut)),
            (1, gateup, (1, slice(None), cut)),
            (2, down, (slice(None), cut)),
        ):
            gradient = mlp_g[:, at + slot * block : at + (slot + 1) * block]
            step(group, index, gradient.astype(jnp.float32))
    step(bias, slice(None), bias_g[...])
    step(gain, slice(None), gain_g[...])


def adam_all(clip, grads, states, stride, block, rates):
    vmem = pl.BlockSpec(memory_space=pltpu.VMEM)
    return pl.pallas_call(
        partial(adam_kernel, stride, block, rates),
        in_specs=[pl.BlockSpec(memory_space=pltpu.SMEM)] + [vmem] * (len(grads) + len(states)),
        out_shape=[jax.ShapeDtypeStruct(x.shape, x.dtype) for x in states],
        compiler_params=pltpu.CompilerParams(vmem_limit_bytes=60 * 1024 * 1024),
    )(clip.reshape(1, 1), *grads, *states)


def padded(columns):
    return -(-columns // 128) * 128


def local(
    tokens,
    cotangent,
    lengths,
    grid_width,
    timestep,
    class_id,
    class_table,
    ada_weight,
    ada_m,
    ada_v,
    ada_bias,
    bias_m,
    bias_v,
    qkv_weight,
    qkv_m,
    qkv_v,
    out_weight,
    out_m,
    out_v,
    gateup_weight,
    gateup_m,
    gateup_v,
    down_weight,
    down_m,
    down_v,
    qk_gain,
    gain_m,
    gain_v,
):
    tensor_count = lax.axis_size("tensor")
    data_count = lax.axis_size("dp")
    tensor_rank = lax.axis_index("tensor")
    data_rank = lax.axis_index("dp")
    local_rows, model_width = tokens.shape
    group_rows = local_rows * tensor_count
    column_share = model_width // tensor_count
    row_share = ada_weight.shape[0]
    head_size = qk_gain.shape[1]
    item_count = lengths.shape[1]
    class_count = class_table.shape[0]
    hidden_share = down_weight.shape[1]
    bf16 = jnp.bfloat16

    stride = padded(column_share)
    block = 256 if hidden_share % 512 == 0 else hidden_share
    blocks = hidden_share // block
    swap = lambda values: jnp.transpose(values, (1, 0, 2))
    attn_shard, mlp_shard = pack(
        swap(qkv_weight), out_weight, swap(gateup_weight), down_weight, stride, block
    )

    ids = gather_rows(jnp.stack([class_id[0], timestep[0]])[None])
    ids, attn_shard = gated(ids, attn_shard)
    item_ids = ids[:, 0].reshape(-1)
    item_steps = ids[:, 1].reshape(-1)
    class_onehot = (
        item_ids[:, None] == jnp.arange(class_count, dtype=jnp.int32)[None, :]
    ).astype(bf16)
    condition = jnp.dot(class_onehot, class_table, preferred_element_type=jnp.float32) + time_embed(
        item_steps, model_width
    )
    silu_all = jax.nn.silu(condition).astype(bf16)
    silu_own = lax.dynamic_slice_in_dim(silu_all, data_rank * row_share, row_share, 1)
    mod_part = mod_product(silu_own, swap(ada_weight), stride)
    half_items = data_count * item_count // 2
    mod_share = reduce_rows(mod_part[:half_items], mod_part[half_items:])
    mod_share = mod_share.reshape(item_count, 6, stride)[:, :, :column_share]
    bias_share = lax.dynamic_slice_in_dim(ada_bias, tensor_rank * column_share, column_share, 1)
    mod_share = mod_share + bias_share[None]
    if tensor_count == 2:
        mod_other = tensor_send(mod_share, 1)
        lower = jnp.where(tensor_rank == 0, mod_share, mod_other)
        upper = jnp.where(tensor_rank == 0, mod_other, mod_share)
        modulation = jnp.concatenate([lower, upper], axis=2)
    else:
        modulation = lax.all_gather(mod_share, "tensor", axis=2, tiled=True)
    tokens_all = tensor_gather(tokens)
    cot_all = tensor_gather(cotangent)
    base_rows = tokens_all.astype(jnp.float32)
    row_blocks = (tensor_rank - jnp.arange(tensor_count, dtype=jnp.int32)) % tensor_count
    row_index = (
        row_blocks[:, None] * local_rows + jnp.arange(local_rows, dtype=jnp.int32)[None, :]
    ).reshape(-1)
    segment, grid_row, grid_col = layout(lengths[0], grid_width[0], row_index)
    tables = rope_tables(grid_row, grid_col, head_size)

    def mod_rows(slot, count):
        picked = modulation[0, slot][None, :]
        for item in range(1, item_count):
            picked = jnp.where(
                segment[:count, None] == item, modulation[item, slot][None, :], picked
            )
        return picked

    def mod_sums(values):
        own = segment[:local_rows]
        return jnp.stack(
            [
                jnp.sum(jnp.where(own[:, None] == item, values, 0.0), axis=0)
                for item in range(item_count)
            ]
        )

    full_attn = lax.all_gather(attn_shard, "dp", axis=0, tiled=True)
    full_mlp = lax.all_gather(mlp_shard, "dp", axis=0, tiled=True)
    full_qkv = full_attn[:, : 3 * stride]
    full_out = full_attn[:, 3 * stride : 3 * stride + column_share]

    attn_in = modulate_in(base_rows, mod_rows(1, group_rows), mod_rows(0, group_rows))
    attn_in = by_rows(attn_in.astype(bf16))
    qkv_raw = jnp.dot(attn_in, full_qkv, preferred_element_type=jnp.float32)
    raw_query, raw_key, raw_value = [
        qkv_raw[:, slot * stride : slot * stride + column_share] for slot in range(3)
    ]
    query_rot, key_rot = qk_prepare(raw_query, raw_key, qk_gain, tables)
    query_low = query_rot.astype(bf16)
    key_low = key_rot.astype(bf16)
    value_low = raw_value.reshape(group_rows, -1, head_size).astype(bf16)
    attn_vals, log_sums = attend(query_low, key_low, value_low, segment)
    attn_low = attn_vals.reshape(group_rows, column_share).astype(bf16)
    branch = jnp.einsum("gc,dc->gd", attn_low, full_out, preferred_element_type=jnp.float32)
    branch, cot_all = gated(by_rows(branch.astype(bf16)), cot_all)
    cot_rows = cot_all.astype(jnp.float32)
    branch = tensor_total(branch)
    mid_rows = base_rows + mod_rows(2, group_rows) * branch
    scale_two = mod_rows(4, group_rows)
    mlp_in = modulate_in(mid_rows, scale_two, mod_rows(3, group_rows)).astype(bf16)
    gate_two = mod_rows(5, group_rows)
    d_branch_mlp = (gate_two * cot_rows).astype(bf16)

    if group_rows <= 512:
        out_part, in_part, g_mlp = mlp_part(mlp_in, d_branch_mlp, full_mlp, blocks)
    else:
        out_part, in_part, g_mlp = mlp_plain(mlp_in, d_branch_mlp, full_mlp, blocks)
    sum_mlp = lax.psum_scatter(g_mlp, "dp", scatter_dimension=0, tiled=True)
    d_mlp_in = tensor_total(in_part)
    branch_mlp = tensor_reduce(out_part)
    out_rows = mid_rows[:local_rows] + gate_two[:local_rows] * branch_mlp
    out_tokens = out_rows.astype(bf16)

    d_mid_norm, d_scale_two, d_shift_two = jax.vjp(
        modulate_in, mid_rows, scale_two, jnp.zeros_like(mid_rows)
    )[1](d_mlp_in)
    d_mid = cot_rows + d_mid_norm
    d_branch_attn = by_rows((mod_rows(2, group_rows) * d_mid).astype(bf16))
    g_out = jnp.einsum("gd,gc->dc", d_branch_attn, attn_low, preferred_element_type=jnp.float32)
    sum_out = fold_rows(g_out.astype(bf16))
    d_attn = jnp.einsum("gd,dc->gc", d_branch_attn, full_out, preferred_element_type=jnp.float32)
    d_attn = d_attn.astype(bf16).reshape(query_low.shape)
    d_query_rot, d_key_rot, d_values = attend_back(
        query_low, key_low, value_low, d_attn, log_sums, segment
    )
    _, pull_qk = jax.vjp(partial(qk_prepare, tables=tables), raw_query, raw_key, qk_gain)
    d_query_raw, d_key_raw, g_gain = pull_qk((d_query_rot, d_key_rot))
    spare = jnp.zeros((group_rows, stride - column_share), jnp.float32)
    d_qkv_low = jnp.concatenate(
        [d_query_raw, spare, d_key_raw, spare, d_values.reshape(group_rows, -1), spare], axis=1
    ).astype(bf16)
    d_attn_part = jnp.einsum("gc,dc->gd", d_qkv_low, full_qkv, preferred_element_type=jnp.float32)
    d_attn_in = tensor_reduce(by_rows(d_attn_part.astype(bf16)))
    g_qkv = jnp.einsum("gd,gc->dc", attn_in, d_qkv_low, preferred_element_type=jnp.float32)
    sum_qkv = fold_rows(g_qkv.astype(bf16))

    own_scale = mod_rows(1, local_rows)
    d_base_norm, d_scale_one, d_shift_one = jax.vjp(
        modulate_in, base_rows[:local_rows], own_scale, jnp.zeros_like(own_scale)
    )[1](d_attn_in)
    input_grad = (d_mid[:local_rows] + d_base_norm).astype(bf16)
    d_mod_part = jnp.stack(
        [
            mod_sums(d_shift_one),
            mod_sums(d_scale_one),
            mod_sums(d_mid[:local_rows] * branch[:local_rows]),
            mod_sums(d_shift_two[:local_rows]),
            mod_sums(d_scale_two[:local_rows]),
            mod_sums(cot_rows[:local_rows] * branch_mlp),
        ],
        axis=1,
    )
    if tensor_count == 2:
        lower, upper = d_mod_part[:, :, :column_share], d_mod_part[:, :, column_share:]
        theirs = jnp.where(tensor_rank == 0, upper, lower)
        d_mod = jnp.where(tensor_rank == 0, lower, upper) + tensor_send(theirs, 1)
    else:
        d_mod = lax.psum_scatter(d_mod_part, "tensor", scatter_dimension=2, tiled=True)
    d_mod = jnp.pad(d_mod, ((0, 0), (0, 0), (0, stride - column_share)))
    d_mod_all = gather_rows(d_mod.reshape(item_count, 6 * stride))
    sum_ada = lax.dot_general(
        silu_own.astype(jnp.float32),
        d_mod_all,
        (((0,), (0,)), ((), ())),
        precision=PRECISE,
        preferred_element_type=jnp.float32,
    )
    bias_share = jnp.sum(d_mod_all, axis=0).reshape(6, stride)[:, :column_share]
    if tensor_count == 2:
        bias_other = tensor_send(bias_share, 1)
        lower = jnp.where(tensor_rank == 0, bias_share, bias_other)
        upper = jnp.where(tensor_rank == 0, bias_other, bias_share)
        bias_grad = jnp.concatenate([lower, upper], axis=1)
    else:
        bias_grad = lax.all_gather(bias_share, "tensor", axis=1, tiled=True)

    local_squares = jnp.sum(sum_ada * sum_ada) + jnp.sum(sum_qkv * sum_qkv)
    local_squares = local_squares + jnp.sum(sum_out * sum_out)
    local_squares = local_squares + jnp.sum(jnp.square(sum_mlp.astype(jnp.float32)))
    packet = jnp.concatenate(
        [
            g_gain.reshape(-1),
            local_squares[None],
            jnp.zeros((256 - 2 * head_size - 1,), jnp.float32),
        ]
    ).reshape(2, 128)
    packet = everywhere_sum(packet).reshape(-1)
    gain_total = packet[: 2 * head_size].reshape(2, head_size)
    grad_norm = jnp.sqrt(
        packet[2 * head_size] + jnp.sum(gain_total * gain_total) + jnp.sum(bias_grad * bias_grad)
    )
    tokens_all_count = local_rows * tensor_count * data_count
    params_all = 10 * D * D + 3 * D * FF + 6 * D + 2 * HD
    limit = 0.01 * math.sqrt(tokens_all_count * params_all)
    clip = limit / jnp.maximum(grad_norm, limit)
    matrix_rate = model_width ** (-0.5)

    out_rate = (model_width // 64) ** (-0.5)
    rates = (matrix_rate, SMALL_RATE, matrix_rate, out_rate, matrix_rate, FF ** (-0.5), SMALL_RATE)
    states = []
    for group in (
        (ada_weight, ada_m, ada_v),
        (ada_bias, bias_m, bias_v),
        (qkv_weight, qkv_m, qkv_v),
        (out_weight, out_m, out_v),
        (gateup_weight, gateup_m, gateup_v),
        (down_weight, down_m, down_v),
        (qk_gain, gain_m, gain_v),
    ):
        states += [swap(x) if x.ndim == 3 else x for x in group]
    grads = [sum_ada, sum_qkv, sum_out, sum_mlp, bias_grad, gain_total]
    updated = adam_all(clip, grads, states, stride, block, rates)
    updated = [swap(x) if x.ndim == 3 else x for x in updated]
    return (
        out_tokens,
        input_grad,
        grad_norm,
        *updated,
    )


def solution(mesh):
    in_specs = (
        P(("dp", "tensor"), None),
        P(("dp", "tensor"), None),
        P("dp", None),
        P("dp", None),
        P("dp", None),
        P("dp", None),
        P(),
        P("dp", None, "tensor"),
        P("dp", None, "tensor"),
        P("dp", None, "tensor"),
        P(),
        P(),
        P(),
        P("dp", None, "tensor"),
        P("dp", None, "tensor"),
        P("dp", None, "tensor"),
        P("dp", "tensor"),
        P("dp", "tensor"),
        P("dp", "tensor"),
        P("dp", None, "tensor"),
        P("dp", None, "tensor"),
        P("dp", None, "tensor"),
        P("dp", "tensor"),
        P("dp", "tensor"),
        P("dp", "tensor"),
        P(),
        P(),
        P(),
    )
    out_specs = (
        P(("dp", "tensor"), None),
        P(("dp", "tensor"), None),
        P(),
        P("dp", None, "tensor"),
        P("dp", None, "tensor"),
        P("dp", None, "tensor"),
        P(),
        P(),
        P(),
        P("dp", None, "tensor"),
        P("dp", None, "tensor"),
        P("dp", None, "tensor"),
        P("dp", "tensor"),
        P("dp", "tensor"),
        P("dp", "tensor"),
        P("dp", None, "tensor"),
        P("dp", None, "tensor"),
        P("dp", None, "tensor"),
        P("dp", "tensor"),
        P("dp", "tensor"),
        P("dp", "tensor"),
        P(),
        P(),
        P(),
    )
    return jax.shard_map(local, mesh=mesh, in_specs=in_specs, out_specs=out_specs, check_vma=False)
```

```python
from functools import partial
import math

import jax
import jax.numpy as jnp
from jax import lax
from jax.experimental import pallas as pl
from jax.experimental.layout import Layout, with_layout_constraint
from jax.experimental.pallas import tpu as pltpu
from jax.sharding import PartitionSpec as P

D = 1152
HD = 72
FF = 3072
STEP = 10


EPSILON = 1e-06
NEG_FILL = -1e30
PRECISE = lax.Precision.HIGHEST
BETA_FIRST = 0.9
BETA_SECOND = 0.95
ADAM_EPSILON = 1e-08
DECAY_RATE = 0.01
SMALL_RATE = 0.5


def rms_scaled(values):
    return values * lax.rsqrt(jnp.mean(values * values, axis=-1, keepdims=True) + EPSILON)


def modulate_in(base_rows, scale_rows, shift_rows):
    return rms_scaled(base_rows) * (1.0 + scale_rows) + shift_rows


def time_embed(step_ids, width):
    half_width = width // 2
    frequency = jnp.exp(-math.log(10000.0) * jnp.arange(half_width, dtype=jnp.float32) / half_width)
    angles = step_ids.astype(jnp.float32)[..., None] * frequency
    return jnp.concatenate([jnp.cos(angles), jnp.sin(angles)], axis=-1)


def layout(item_lengths, item_widths, row_index):
    ends_at = jnp.cumsum(item_lengths)
    starts_at = ends_at - item_lengths
    segment = jnp.sum((row_index[:, None] >= ends_at[None, :]).astype(jnp.int32), axis=1)
    member = segment[:, None] == jnp.arange(item_lengths.shape[0], dtype=jnp.int32)[None, :]
    offset = jnp.sum(jnp.where(member, starts_at[None, :], 0), axis=1)
    grid_span = jnp.sum(jnp.where(member, item_widths[None, :], 0), axis=1)
    inside = row_index - offset
    return (segment, inside // grid_span, inside % grid_span)


def rope_tables(grid_row, grid_col, head_size):
    quarter = head_size // 4
    frequency = jnp.exp(-math.log(10000.0) * jnp.arange(quarter, dtype=jnp.float32) / quarter)
    row_angle = grid_row.astype(jnp.float32)[:, None] * frequency[None, :]
    col_angle = grid_col.astype(jnp.float32)[:, None] * frequency[None, :]
    return (jnp.cos(row_angle), jnp.sin(row_angle), jnp.cos(col_angle), jnp.sin(col_angle))


def turn_half(part, cosine, sine):
    quarter = part.shape[-1] // 2
    first_part = part[..., :quarter]
    second_part = part[..., quarter:]
    cosine = cosine[:, None, :]
    sine = sine[:, None, :]
    return jnp.concatenate(
        [first_part * cosine - second_part * sine, first_part * sine + second_part * cosine],
        axis=-1,
    )


def rotate(values, tables):
    half_size = values.shape[-1] // 2
    return jnp.concatenate(
        [
            turn_half(values[..., :half_size], tables[0], tables[1]),
            turn_half(values[..., half_size:], tables[2], tables[3]),
        ],
        axis=-1,
    )


def qk_prepare(raw_query, raw_key, gains, tables):
    head_size = gains.shape[1]
    row_count = raw_query.shape[0]
    head_count = raw_query.shape[1] // head_size
    query_norm = rms_scaled(raw_query.reshape(row_count, head_count, head_size)) * gains[0]
    key_norm = rms_scaled(raw_key.reshape(row_count, head_count, head_size)) * gains[1]
    return (rotate(query_norm, tables), rotate(key_norm, tables))


def block_geometry(total_rows):
    query_block = min(512, total_rows)
    return (query_block, total_rows, total_rows // query_block)


def window_start(block_index, query_block, key_window, total_rows):
    return jnp.clip(block_index * query_block - query_block, 0, total_rows - key_window)


def masked_scores(query_low, key_low, segment, block_index, query_block, key_window):
    total_rows = query_low.shape[0]
    scale = query_low.shape[2] ** (-0.5)
    query_start = block_index * query_block
    key_start = window_start(block_index, query_block, key_window, total_rows)
    queries = lax.dynamic_slice_in_dim(query_low, query_start, query_block, 0)
    seg_query = lax.dynamic_slice_in_dim(segment, query_start, query_block, 0)
    scores = (
        jnp.einsum("qhe,khe->hqk", queries, key_low, preferred_element_type=jnp.float32) * scale
    )
    allowed = (seg_query[:, None] == segment[None, :])[None]
    return (jnp.where(allowed, scores, NEG_FILL), queries, key_low, query_start, key_start)


def attend(query_low, key_low, value_low, segment):
    total_rows = query_low.shape[0]
    query_block, key_window, block_count = block_geometry(total_rows)

    def one_block(block_index):
        scores, queries, keyset, query_start, key_start = masked_scores(
            query_low, key_low, segment, block_index, query_block, key_window
        )
        peak = jnp.max(scores, axis=-1, keepdims=True)
        expo = jnp.exp(scores - peak)
        total_exp = jnp.sum(expo, axis=-1, keepdims=True)
        probs = (expo / total_exp).astype(jnp.bfloat16)
        result = jnp.einsum("hqk,khe->qhe", probs, value_low, preferred_element_type=jnp.float32)
        return (result, (peak + jnp.log(total_exp))[..., 0])

    outputs, log_sums = lax.map(one_block, jnp.arange(block_count, dtype=jnp.int32))
    return (outputs.reshape(total_rows, query_low.shape[1], query_low.shape[2]), log_sums)


def attend_back(query_low, key_low, value_low, d_attn, log_sums, segment):
    total_rows = query_low.shape[0]
    query_block, key_window, block_count = block_geometry(total_rows)
    scale = query_low.shape[2] ** (-0.5)
    zeros_like = jnp.zeros(query_low.shape, jnp.float32)

    def one_block(carry, block_index):
        d_keys, d_values = carry
        scores, queries, keyset, query_start, key_start = masked_scores(
            query_low, key_low, segment, block_index, query_block, key_window
        )
        grads_block = lax.dynamic_slice_in_dim(d_attn, query_start, query_block, 0)
        probs = jnp.exp(scores - log_sums[block_index][:, :, None])
        low_probs = probs.astype(jnp.bfloat16)
        d_probs = jnp.einsum(
            "qhe,khe->hqk", grads_block, value_low, preferred_element_type=jnp.float32
        )
        row_dot = jnp.sum(probs * d_probs, axis=-1, keepdims=True)
        d_scores = (probs * (d_probs - row_dot)).astype(jnp.bfloat16)
        d_query = (
            jnp.einsum("hqk,khe->qhe", d_scores, keyset, preferred_element_type=jnp.float32) * scale
        )
        d_key_part = (
            jnp.einsum("hqk,qhe->khe", d_scores, queries, preferred_element_type=jnp.float32)
            * scale
        )
        d_value_part = jnp.einsum(
            "hqk,qhe->khe", low_probs, grads_block, preferred_element_type=jnp.float32
        )
        d_keys = d_keys + d_key_part
        d_values = d_values + d_value_part
        return ((d_keys, d_values), d_query)

    (d_keys, d_values), d_queries = lax.scan(
        one_block, (zeros_like, zeros_like), jnp.arange(block_count, dtype=jnp.int32)
    )
    return (d_queries.reshape(query_low.shape), d_keys, d_values)


def adam_update(weight, first_moment, second_moment, gradient, rate, clip):
    clipped = gradient * clip
    new_first = BETA_FIRST * first_moment + (1.0 - BETA_FIRST) * clipped
    new_second = BETA_SECOND * second_moment + (1.0 - BETA_SECOND) * clipped * clipped
    unbiased_first = new_first / (1.0 - BETA_FIRST**STEP)
    unbiased_second = new_second / (1.0 - BETA_SECOND**STEP)
    new_weight = weight - rate * (
        unbiased_first / (jnp.sqrt(unbiased_second) + ADAM_EPSILON) + DECAY_RATE * weight
    )
    return (new_weight, new_first, new_second)


ZSIDE = 4
CORES = 2


def place_of(rank, count):
    xside = count // (ZSIDE * CORES)
    return (rank // (xside * CORES), (rank // CORES) % xside, rank % CORES)


def shift_pairs(count, dim, amount):
    xside = count // (ZSIDE * CORES)
    pairs = []
    for rank in range(count):
        z, x, core = place_of(rank, count)
        if dim == "z":
            z = (z + amount) % ZSIDE
        elif dim == "x":
            x = (x + amount) % xside
        else:
            core = (core + amount) % CORES
        pairs.append((rank, (z * xside + x) * CORES + core))
    return pairs


def send(values, dim, amount):
    count = lax.axis_size("dp")
    return lax.ppermute(values, "dp", shift_pairs(count, dim, amount))


def tensor_send(values, amount):
    count = lax.axis_size("tensor")
    return lax.ppermute(values, "tensor", [(r, (r + amount) % count) for r in range(count)])


def block_order(rank, count):
    xside = count // (ZSIDE * CORES)
    z, x, core = place_of(rank, count)
    flips = jnp.arange(CORES, dtype=jnp.int32)[:, None, None]
    turns = jnp.arange(xside, dtype=jnp.int32)[None, :, None]
    hops = jnp.arange(ZSIDE, dtype=jnp.int32)[None, None, :]
    their_z = (z - hops) % ZSIDE
    their_x = (x - turns) % xside
    their_core = (core + flips) % CORES
    return ((their_z * xside + their_x) * CORES + their_core).reshape(count)


def near_rows(shard):
    return jnp.concatenate([shard] + [send(shard, "z", hop) for hop in range(1, ZSIDE)], axis=0)


def far_rows(near):
    xside = lax.axis_size("dp") // (ZSIDE * CORES)
    mine = jnp.concatenate([near] + [send(near, "x", turn) for turn in range(1, xside)], axis=0)
    return jnp.concatenate([mine, send(mine, "core", 1)], axis=0)


def gather_rows(shard):
    return far_rows(near_rows(shard))


def by_rows(values):
    return with_layout_constraint(values, Layout(tuple(range(values.ndim))))


def gated(value, gate):
    return lax.optimization_barrier((value, gate))


def fold_core(mine, other):
    parts = []
    for own, theirs in zip(mine, other):
        came = send(theirs, "core", 1)
        parts.append((own.astype(jnp.float32) + came.astype(jnp.float32)).astype(own.dtype))
    return parts


def fold_x(parts):
    z = place_of(lax.axis_index("dp"), lax.axis_size("dp"))[0]
    total = parts[0].astype(jnp.float32)
    for turn in range(1, len(parts)):
        total = total + send(parts[turn], "x", -turn).astype(jnp.float32)
    total = total.astype(parts[0].dtype)
    return [
        lax.dynamic_index_in_dim(total, (z - hop) % ZSIDE, 0, keepdims=False) for hop in range(ZSIDE)
    ]


def fold_z(cuts):
    total = cuts[0].astype(jnp.float32)
    for hop in range(1, ZSIDE):
        total = total + send(cuts[hop], "z", -hop).astype(jnp.float32)
    return total


def reduce_rows(mine, other):
    xside = lax.axis_size("dp") // (ZSIDE * CORES)
    total = mine + send(other, "core", 1)
    for side, count in (("x", xside), ("z", ZSIDE)):
        rows = total.shape[0] // count
        cuts = [total[turn * rows : (turn + 1) * rows] for turn in range(count)]
        total = cuts[0]
        for turn in range(1, count):
            total = total + send(cuts[turn], side, -turn)
    return total


def split_core(gradient):
    count = lax.axis_size("dp")
    xside = count // (ZSIDE * CORES)
    z, x, core = place_of(lax.axis_index("dp"), count)
    rows = gradient.shape[0] // count
    blocks = gradient.reshape(ZSIDE, xside, CORES, rows, -1)
    halves = []
    for side in (core, 1 - core):
        half = lax.dynamic_index_in_dim(blocks, side, 2, keepdims=False)
        turns = [(x - turn) % xside for turn in range(xside)]
        cut = [lax.dynamic_index_in_dim(half, turn, 1, keepdims=False) for turn in turns]
        halves.append(cut)
    return halves


def tensor_gather(values):
    count = lax.axis_size("tensor")
    return jnp.concatenate([values] + [tensor_send(values, hop) for hop in range(1, count)], axis=0)


def tensor_reduce(values):
    count = lax.axis_size("tensor")
    rows = values.shape[0] // count
    total = values[:rows].astype(jnp.float32)
    for hop in range(1, count):
        came = tensor_send(values[hop * rows : (hop + 1) * rows], -hop)
        total = total + came.astype(jnp.float32)
    return total


def tensor_total(values):
    count = lax.axis_size("tensor")
    if count == 2:
        half = values.shape[0] // 2
        came = tensor_send(values, 1)
        came = jnp.concatenate([came[half:], came[:half]], axis=0)
        return values.astype(jnp.float32) + came.astype(jnp.float32)
    return tensor_gather(tensor_reduce(values).astype(values.dtype)).astype(jnp.float32)


def everywhere_sum(values):
    for axis in ("dp", "tensor"):
        count = lax.axis_size(axis)
        step = 1
        while step < count:
            values = values + lax.ppermute(values, axis, [(r, r ^ step) for r in range(count)])
            step *= 2
    return values


def mlp_kernel(rows_ref, grad_ref, held, out_ref, in_ref, act_ref, out_acc, in_acc):
    step = pl.program_id(0)
    width = held.shape[1] // 3
    gate_w = held[:, :width]
    up_w = held[:, width : 2 * width]
    down_w = held[:, 2 * width :]

    @pl.when(step == 0)
    def _():
        out_acc[...] = jnp.zeros_like(out_acc)
        in_acc[...] = jnp.zeros_like(in_acc)

    across = (((1,), (1,)), ((), ()))
    gate = jnp.dot(rows_ref[...], gate_w, preferred_element_type=jnp.float32)
    up = jnp.dot(rows_ref[...], up_w, preferred_element_type=jnp.float32)
    d_hidden = jnp.dot(grad_ref[...], down_w, preferred_element_type=jnp.float32)
    sigmoid = 1.0 / (1.0 + jnp.exp(-gate))
    silu = gate * sigmoid
    hidden = (silu * up).astype(jnp.bfloat16)
    d_gate = (d_hidden * up * sigmoid * (1.0 + gate * (1.0 - sigmoid))).astype(jnp.bfloat16)
    d_up = (d_hidden * silu).astype(jnp.bfloat16)
    act_ref[:, :width] = d_gate
    act_ref[:, width : 2 * width] = d_up
    act_ref[:, 2 * width :] = hidden
    out_acc[...] += lax.dot_general(hidden, down_w, across, preferred_element_type=jnp.float32)
    in_acc[...] += lax.dot_general(
        d_gate, gate_w, across, preferred_element_type=jnp.float32
    ) + lax.dot_general(d_up, up_w, across, preferred_element_type=jnp.float32)

    @pl.when(step == pl.num_programs(0) - 1)
    def _():
        out_ref[...] = out_acc[...].astype(out_ref.dtype)
        in_ref[...] = in_acc[...].astype(in_ref.dtype)


def mlp_part(rows, grad, weights, blocks):
    count, width = rows.shape
    columns = weights.shape[1]
    block = columns // blocks
    whole = pl.BlockSpec((count, width), lambda i: (0, 0))
    across = pl.BlockSpec((width, block), lambda i: (0, i))
    acts = pl.BlockSpec((count, block), lambda i: (0, i))
    return pl.pallas_call(
        mlp_kernel,
        grid=(blocks,),
        in_specs=[whole, whole, across],
        out_specs=[whole, whole, acts],
        out_shape=[jax.ShapeDtypeStruct((count, width), jnp.bfloat16)] * 2
        + [jax.ShapeDtypeStruct((count, columns), jnp.bfloat16)],
        scratch_shapes=[pltpu.VMEM((count, width), jnp.float32)] * 2,
        cost_estimate=pl.CostEstimate(
            flops=4 * count * width * columns,
            bytes_accessed=2 * width * columns,
            transcendentals=count * columns // 3,
        ),
        compiler_params=pltpu.CompilerParams(vmem_limit_bytes=60 * 1024 * 1024),
    )(rows, grad, weights)


def grad_kernel(rows_t_ref, grad_t_ref, *refs):
    acts, target = refs[:-1], refs[-1]
    width = target.shape[1] // 3
    for at, left in ((0, rows_t_ref), (width, rows_t_ref), (2 * width, grad_t_ref)):
        cut = slice(at, at + width)
        begin = 0
        product = None
        for act_ref in acts:
            rows = slice(begin, begin + act_ref.shape[0])
            share = jnp.dot(left[:, rows], act_ref[:, cut], preferred_element_type=jnp.float32)
            product = share if product is None else product + share
            begin = rows.stop
        target[:, cut] = product.astype(target.dtype)


def grad_part(rows_t, grad_t, acts, blocks):
    width, count = rows_t.shape
    columns = acts[0].shape[1]
    block = columns // blocks
    whole = pl.BlockSpec((width, count), lambda i: (0, 0))
    return pl.pallas_call(
        grad_kernel,
        grid=(blocks,),
        in_specs=[whole, whole]
        + [pl.BlockSpec((act.shape[0], block), lambda i: (0, i)) for act in acts],
        out_specs=pl.BlockSpec((width, block), lambda i: (0, i)),
        out_shape=jax.ShapeDtypeStruct((width, columns), jnp.bfloat16),
        cost_estimate=pl.CostEstimate(
            flops=2 * count * width * columns, bytes_accessed=2 * width * columns, transcendentals=0
        ),
        compiler_params=pltpu.CompilerParams(vmem_limit_bytes=60 * 1024 * 1024),
    )(rows_t, grad_t, *acts)


def mlp_plain(rows, grad, weights, blocks):
    width = weights.shape[0]
    block = weights.shape[1] // (3 * blocks)
    split = weights.reshape(width, blocks, 3, block)
    gate_w, up_w, down_w = [split[:, :, slot].reshape(width, blocks * block) for slot in range(3)]
    gate = jnp.dot(rows, gate_w, preferred_element_type=jnp.float32)
    up = jnp.dot(rows, up_w, preferred_element_type=jnp.float32)
    d_hidden = jnp.dot(grad, down_w, preferred_element_type=jnp.float32)
    sigmoid = jax.nn.sigmoid(gate)
    hidden = (gate * sigmoid * up).astype(jnp.bfloat16)
    d_gate = (d_hidden * up * sigmoid * (1.0 + gate * (1.0 - sigmoid))).astype(jnp.bfloat16)
    d_up = (d_hidden * gate * sigmoid).astype(jnp.bfloat16)
    out_sum = jnp.dot(hidden, down_w.T, preferred_element_type=jnp.float32)
    in_sum = jnp.dot(d_gate, gate_w.T, preferred_element_type=jnp.float32) + jnp.dot(
        d_up, up_w.T, preferred_element_type=jnp.float32
    )
    grads = [
        jnp.einsum("gd,gf->df", left, right, preferred_element_type=jnp.float32)
        .astype(jnp.bfloat16)
        .reshape(width, blocks, block)
        for left, right in ((rows, d_gate), (rows, d_up), (grad, hidden))
    ]
    packed = jnp.stack(grads, axis=2).reshape(width, 3 * blocks * block)
    return (out_sum.astype(jnp.bfloat16), in_sum.astype(jnp.bfloat16), packed)


def pack_attn_kernel(qkv_ref, out_ref, target):
    columns = out_ref.shape[1]
    for slot in range(3):
        target[:, slot * columns : (slot + 1) * columns] = qkv_ref[slot].astype(target.dtype)
    target[:, 3 * columns :] = out_ref[...].astype(target.dtype)


def pack_attn(qkv, out):
    rows, columns = out.shape
    return pl.pallas_call(
        pack_attn_kernel, out_shape=jax.ShapeDtypeStruct((rows, 4 * columns), jnp.bfloat16)
    )(qkv, out)


def pack_mlp_kernel(block, gateup_ref, down_ref, target):
    for begin in range(0, down_ref.shape[1], block):
        cut = slice(begin, begin + block)
        at = 3 * begin
        target[:, at : at + block] = gateup_ref[0, :, cut].astype(target.dtype)
        target[:, at + block : at + 2 * block] = gateup_ref[1, :, cut].astype(target.dtype)
        target[:, at + 2 * block : at + 3 * block] = down_ref[:, cut].astype(target.dtype)


def pack_mlp(gateup, down, block):
    rows, hidden = down.shape
    return pl.pallas_call(
        partial(pack_mlp_kernel, block),
        out_shape=jax.ShapeDtypeStruct((rows, 3 * hidden), jnp.bfloat16),
    )(gateup, down)


def mod_kernel(stride, rows_ref, ada_ref, target):
    columns = ada_ref.shape[2]
    target[...] = jnp.zeros_like(target)
    for slot in range(ada_ref.shape[0]):
        target[:, slot * stride : slot * stride + columns] = jnp.dot(
            rows_ref[...], ada_ref[slot].astype(jnp.bfloat16), preferred_element_type=jnp.float32
        )


def mod_product(rows, ada, stride):
    return pl.pallas_call(
        partial(mod_kernel, stride),
        out_shape=jax.ShapeDtypeStruct((rows.shape[0], ada.shape[0] * stride), jnp.float32),
    )(rows, ada)


def adam_kernel(rates, clip_ref, *refs):
    clip = clip_ref[0, 0]
    count = len(rates)
    grads, states, targets = refs[:count], refs[count : 4 * count], refs[4 * count :]
    for index, rate in enumerate(rates):
        held = states[3 * index : 3 * index + 3]
        put = targets[3 * index : 3 * index + 3]
        paired = len(grads[index].shape) == 3 and grads[index].shape[1] == 2
        rows = grads[index].shape[0 if paired else -2]
        tall = 8 if rows % 8 == 0 else rows

        def step(
            at, carry, held=held, put=put, source=grads[index], rate=rate, tall=tall, paired=paired
        ):
            cut = pl.ds(at * tall, tall)
            cell = (cut,) if paired or len(source.shape) == 2 else (slice(None), cut)
            result = adam_update(*[ref[cell] for ref in held], source[cell], rate, clip)
            for ref, value in zip(put, result):
                ref[cell] = value
            return carry

        lax.fori_loop(0, rows // tall, step, 0)


def adam_all(clip, grads, states, rates):
    vmem = pl.BlockSpec(memory_space=pltpu.VMEM)
    return pl.pallas_call(
        partial(adam_kernel, rates),
        in_specs=[pl.BlockSpec(memory_space=pltpu.SMEM)] + [vmem] * (len(grads) + len(states)),
        out_shape=[jax.ShapeDtypeStruct(x.shape, x.dtype) for x in states],
        compiler_params=pltpu.CompilerParams(vmem_limit_bytes=60 * 1024 * 1024),
    )(clip.reshape(1, 1), *grads, *states)


def padded(columns):
    return -(-columns // 128) * 128


def local(
    tokens,
    cotangent,
    lengths,
    grid_width,
    timestep,
    class_id,
    class_table,
    ada_weight,
    ada_m,
    ada_v,
    ada_bias,
    bias_m,
    bias_v,
    qkv_weight,
    qkv_m,
    qkv_v,
    out_weight,
    out_m,
    out_v,
    gateup_weight,
    gateup_m,
    gateup_v,
    down_weight,
    down_m,
    down_v,
    qk_gain,
    gain_m,
    gain_v,
):
    tensor_count = lax.axis_size("tensor")
    data_count = lax.axis_size("dp")
    tensor_rank = lax.axis_index("tensor")
    data_rank = lax.axis_index("dp")
    local_rows, model_width = tokens.shape
    group_rows = local_rows * tensor_count
    column_share = model_width // tensor_count
    row_share = ada_weight.shape[0]
    head_size = qk_gain.shape[1]
    item_count = lengths.shape[1]
    class_count = class_table.shape[0]
    hidden_share = down_weight.shape[1]
    bf16 = jnp.bfloat16

    stride = padded(column_share)
    block = 256 if hidden_share % 512 == 0 else hidden_share
    blocks = hidden_share // block
    swap = lambda values: jnp.transpose(values, (1, 0, 2))
    attn_shard = pack_attn(swap(qkv_weight), out_weight)
    full_attn = lax.all_gather(attn_shard, "dp", axis=0, tiled=True)
    mlp_shard = pack_mlp(swap(gateup_weight), down_weight, block)
    full_mlp = lax.all_gather(mlp_shard, "dp", axis=0, tiled=True)
    full_qkv = full_attn[:, : 3 * column_share]
    full_out = full_attn[:, 3 * column_share :]

    ids = gather_rows(jnp.stack([class_id[0], timestep[0]])[None])
    item_ids = ids[:, 0].reshape(-1)
    item_steps = ids[:, 1].reshape(-1)
    class_onehot = (
        item_ids[:, None] == jnp.arange(class_count, dtype=jnp.int32)[None, :]
    ).astype(bf16)
    condition = jnp.dot(class_onehot, class_table, preferred_element_type=jnp.float32) + time_embed(
        item_steps, model_width
    )
    silu_all = jax.nn.silu(condition).astype(bf16)
    silu_own = lax.dynamic_slice_in_dim(silu_all, data_rank * row_share, row_share, 1)
    mod_part = mod_product(silu_own, swap(ada_weight), stride)
    half_items = data_count * item_count // 2
    mod_share = reduce_rows(mod_part[:half_items], mod_part[half_items:])
    mod_share = mod_share.reshape(item_count, 6, stride)[:, :, :column_share]
    bias_share = lax.dynamic_slice_in_dim(ada_bias, tensor_rank * column_share, column_share, 1)
    mod_share = mod_share + bias_share[None]
    if tensor_count == 2:
        mod_other = tensor_send(mod_share, 1)
        lower = jnp.where(tensor_rank == 0, mod_share, mod_other)
        upper = jnp.where(tensor_rank == 0, mod_other, mod_share)
        modulation = jnp.concatenate([lower, upper], axis=2)
    else:
        modulation = lax.all_gather(mod_share, "tensor", axis=2, tiled=True)
    tokens_all = by_rows(tensor_gather(tokens))
    cot_all = by_rows(tensor_gather(cotangent))
    base_rows = tokens_all.astype(jnp.float32)
    row_blocks = (tensor_rank - jnp.arange(tensor_count, dtype=jnp.int32)) % tensor_count
    row_index = (
        row_blocks[:, None] * local_rows + jnp.arange(local_rows, dtype=jnp.int32)[None, :]
    ).reshape(-1)
    segment, grid_row, grid_col = layout(lengths[0], grid_width[0], row_index)
    tables = rope_tables(grid_row, grid_col, head_size)

    def mod_rows(slot, count):
        picked = modulation[0, slot][None, :]
        for item in range(1, item_count):
            picked = jnp.where(
                segment[:count, None] == item, modulation[item, slot][None, :], picked
            )
        return picked

    def mod_sums(values):
        own = segment[:local_rows]
        return jnp.stack(
            [
                jnp.sum(jnp.where(own[:, None] == item, values, 0.0), axis=0)
                for item in range(item_count)
            ]
        )

    attn_in = modulate_in(base_rows, mod_rows(1, group_rows), mod_rows(0, group_rows))
    attn_in = by_rows(attn_in.astype(bf16))
    qkv_raw = jnp.dot(attn_in, full_qkv, preferred_element_type=jnp.float32)
    raw_query, raw_key, raw_value = [
        qkv_raw[:, slot * column_share : (slot + 1) * column_share] for slot in range(3)
    ]
    query_rot, key_rot = qk_prepare(raw_query, raw_key, qk_gain, tables)
    query_low = query_rot.astype(bf16)
    key_low = key_rot.astype(bf16)
    value_low = raw_value.reshape(group_rows, -1, head_size).astype(bf16)
    attn_vals, log_sums = attend(query_low, key_low, value_low, segment)
    attn_low = attn_vals.reshape(group_rows, column_share).astype(bf16)
    branch = jnp.einsum("gc,dc->gd", attn_low, full_out, preferred_element_type=jnp.float32)
    branch, cot_all = gated(by_rows(branch.astype(bf16)), cot_all)
    cot_rows = cot_all.astype(jnp.float32)
    branch = by_rows(tensor_total(branch))
    mid_rows = by_rows(base_rows + mod_rows(2, group_rows) * branch)
    scale_two = mod_rows(4, group_rows)
    mlp_in = by_rows(modulate_in(mid_rows, scale_two, mod_rows(3, group_rows)).astype(bf16))
    gate_two = mod_rows(5, group_rows)
    d_branch_mlp = by_rows((gate_two * cot_rows).astype(bf16))

    if group_rows <= 512:
        turned = (mlp_in.T, d_branch_mlp.T)
        (mlp_in, d_branch_mlp), turned = gated((mlp_in, d_branch_mlp), turned)
        out_part, in_part, acts = mlp_part(mlp_in, d_branch_mlp, full_mlp, blocks)
        g_mlp = grad_part(*turned, (acts,), blocks)
    else:
        out_part, in_part, g_mlp = mlp_plain(mlp_in, d_branch_mlp, full_mlp, blocks)
    sum_mlp = lax.psum_scatter(g_mlp, "dp", scatter_dimension=0, tiled=True)
    d_mlp_in = by_rows(tensor_total(in_part))
    branch_mlp = by_rows(tensor_reduce(out_part))
    out_rows = mid_rows[:local_rows] + gate_two[:local_rows] * branch_mlp
    out_tokens = out_rows.astype(bf16)

    d_mid_norm, d_scale_two, d_shift_two = jax.vjp(
        modulate_in, mid_rows, scale_two, jnp.zeros_like(mid_rows)
    )[1](d_mlp_in)
    d_mid = by_rows(cot_rows + d_mid_norm)
    d_branch_attn = by_rows((mod_rows(2, group_rows) * d_mid).astype(bf16))
    d_attn = jnp.einsum("gd,dc->gc", d_branch_attn, full_out, preferred_element_type=jnp.float32)
    d_attn = d_attn.astype(bf16).reshape(query_low.shape)
    d_query_rot, d_key_rot, d_values = attend_back(
        query_low, key_low, value_low, d_attn, log_sums, segment
    )
    _, pull_qk = jax.vjp(partial(qk_prepare, tables=tables), raw_query, raw_key, qk_gain)
    d_query_raw, d_key_raw, g_gain = pull_qk((d_query_rot, d_key_rot))
    d_qkv_low = jnp.concatenate(
        [d_query_raw, d_key_raw, d_values.reshape(group_rows, -1)], axis=1
    ).astype(bf16)
    g_qkv = jnp.einsum("gd,gc->dc", attn_in, d_qkv_low, preferred_element_type=jnp.float32)
    mine, other = split_core(by_rows(g_qkv.astype(bf16)))
    other, d_qkv_low = gated(other, d_qkv_low)
    d_attn_part = jnp.einsum("gc,dc->gd", d_qkv_low, full_qkv, preferred_element_type=jnp.float32)
    turns, d_attn_part = gated(fold_core(mine, other), by_rows(d_attn_part.astype(bf16)))
    d_attn_in = by_rows(tensor_reduce(d_attn_part))
    turns, d_branch_attn = gated(turns, d_branch_attn)
    g_out = jnp.einsum("gd,gc->dc", d_branch_attn, attn_low, preferred_element_type=jnp.float32)
    out_turns = fold_core(*split_core(by_rows(g_out.astype(bf16))))
    qkv_cuts = fold_x(turns)
    qkv_cuts, (d_attn_in, out_turns) = gated(qkv_cuts, (d_attn_in, out_turns))
    sum_qkv = fold_z(qkv_cuts)
    out_cuts = fold_x(out_turns)

    own_scale = mod_rows(1, local_rows)
    d_base_norm, d_scale_one, d_shift_one = jax.vjp(
        modulate_in, base_rows[:local_rows], own_scale, jnp.zeros_like(own_scale)
    )[1](d_attn_in)
    input_grad = (d_mid[:local_rows] + d_base_norm).astype(bf16)
    d_mod_part = jnp.stack(
        [
            mod_sums(d_shift_one),
            mod_sums(d_scale_one),
            mod_sums(d_mid[:local_rows] * branch[:local_rows]),
            mod_sums(d_shift_two[:local_rows]),
            mod_sums(d_scale_two[:local_rows]),
            mod_sums(cot_rows[:local_rows] * branch_mlp),
        ],
        axis=1,
    )
    d_mod_part, out_cuts = gated(d_mod_part, out_cuts)
    sum_out = fold_z(out_cuts)
    if tensor_count == 2:
        lower, upper = d_mod_part[:, :, :column_share], d_mod_part[:, :, column_share:]
        theirs = jnp.where(tensor_rank == 0, upper, lower)
        d_mod = jnp.where(tensor_rank == 0, lower, upper) + tensor_send(theirs, 1)
    else:
        d_mod = lax.psum_scatter(d_mod_part, "tensor", scatter_dimension=2, tiled=True)
    d_mod = jnp.pad(d_mod, ((0, 0), (0, 0), (0, stride - column_share)))
    d_mod_near = near_rows(d_mod.reshape(item_count, 6 * stride))
    d_mod_all = far_rows(d_mod_near)
    sum_ada = lax.dot_general(
        silu_own.astype(jnp.float32),
        d_mod_all,
        (((0,), (0,)), ((), ())),
        precision=PRECISE,
        preferred_element_type=jnp.float32,
    )
    bias_share = jnp.sum(d_mod_all, axis=0).reshape(6, stride)[:, :column_share]
    if tensor_count == 2:
        bias_other = tensor_send(bias_share, 1)
        lower = jnp.where(tensor_rank == 0, bias_share, bias_other)
        upper = jnp.where(tensor_rank == 0, bias_other, bias_share)
        bias_grad = jnp.concatenate([lower, upper], axis=1)
    else:
        bias_grad = lax.all_gather(bias_share, "tensor", axis=1, tiled=True)

    local_squares = jnp.sum(sum_ada * sum_ada) + jnp.sum(sum_qkv * sum_qkv)
    local_squares = local_squares + jnp.sum(bias_share * bias_share) / data_count
    local_squares = local_squares + jnp.sum(sum_out * sum_out)
    local_squares = local_squares + jnp.sum(jnp.square(sum_mlp.astype(jnp.float32)))
    packet = jnp.concatenate(
        [
            g_gain.reshape(-1),
            local_squares[None],
            jnp.zeros((256 - 2 * head_size - 1,), jnp.float32),
        ]
    ).reshape(2, 128)
    packet = everywhere_sum(packet).reshape(-1)
    gain_total = packet[: 2 * head_size].reshape(2, head_size)
    grad_norm = jnp.sqrt(
        packet[2 * head_size] + jnp.sum(gain_total * gain_total)
    )
    tokens_all_count = local_rows * tensor_count * data_count
    params_all = 10 * D * D + 3 * D * FF + 6 * D + 2 * HD
    limit = 0.01 * math.sqrt(tokens_all_count * params_all)
    clip = limit / jnp.maximum(grad_norm, limit)
    matrix_rate = model_width ** (-0.5)

    out_rate = (model_width // 64) ** (-0.5)
    hidden_rate = FF ** (-0.5)
    rates = (matrix_rate, SMALL_RATE, matrix_rate, out_rate, matrix_rate, hidden_rate, SMALL_RATE)
    same = lambda values: values
    views = (
        ((ada_weight, ada_m, ada_v), swap, swap),
        ((ada_bias, bias_m, bias_v), same, same),
        ((qkv_weight, qkv_m, qkv_v), swap, swap),
        ((out_weight, out_m, out_v), same, same),
        ((gateup_weight, gateup_m, gateup_v), same, same),
        ((down_weight, down_m, down_v), same, same),
        ((qk_gain, gain_m, gain_v), same, same),
    )
    by_slot = lambda values, width: jnp.stack(
        [values[:, at : at + column_share] for at in range(0, values.shape[1], width)]
    )
    mlp_split = sum_mlp.reshape(row_share, blocks, 3, block).astype(jnp.float32)
    gateup_grad = jnp.stack(
        [mlp_split[:, :, slot].reshape(row_share, hidden_share) for slot in range(2)], axis=1
    )
    grads = [
        by_slot(sum_ada, stride),
        bias_grad,
        by_slot(sum_qkv, column_share),
        sum_out,
        gateup_grad,
        mlp_split[:, :, 2].reshape(row_share, hidden_share),
        gain_total,
    ]
    states = [view(x) for group, view, _ in views for x in group]
    updated = adam_all(clip, grads, states, rates)
    updated = [
        back(updated[3 * index + slot])
        for index, (_, _, back) in enumerate(views)
        for slot in range(3)
    ]
    return (
        out_tokens,
        input_grad,
        grad_norm,
        *updated,
    )


def solution(mesh):
    in_specs = (
        P(("dp", "tensor"), None),
        P(("dp", "tensor"), None),
        P("dp", None),
        P("dp", None),
        P("dp", None),
        P("dp", None),
        P(),
        P("dp", None, "tensor"),
        P("dp", None, "tensor"),
        P("dp", None, "tensor"),
        P(),
        P(),
        P(),
        P("dp", None, "tensor"),
        P("dp", None, "tensor"),
        P("dp", None, "tensor"),
        P("dp", "tensor"),
        P("dp", "tensor"),
        P("dp", "tensor"),
        P("dp", None, "tensor"),
        P("dp", None, "tensor"),
        P("dp", None, "tensor"),
        P("dp", "tensor"),
        P("dp", "tensor"),
        P("dp", "tensor"),
        P(),
        P(),
        P(),
    )
    out_specs = (
        P(("dp", "tensor"), None),
        P(("dp", "tensor"), None),
        P(),
        P("dp", None, "tensor"),
        P("dp", None, "tensor"),
        P("dp", None, "tensor"),
        P(),
        P(),
        P(),
        P("dp", None, "tensor"),
        P("dp", None, "tensor"),
        P("dp", None, "tensor"),
        P("dp", "tensor"),
        P("dp", "tensor"),
        P("dp", "tensor"),
        P("dp", None, "tensor"),
        P("dp", None, "tensor"),
        P("dp", None, "tensor"),
        P("dp", "tensor"),
        P("dp", "tensor"),
        P("dp", "tensor"),
        P(),
        P(),
        P(),
    )
    return jax.shard_map(local, mesh=mesh, in_specs=in_specs, out_specs=out_specs, check_vma=False)
```

```python
from functools import partial
import math

import jax
import jax.numpy as jnp
from jax import lax
from jax.experimental import pallas as pl
from jax.experimental.layout import Layout, with_layout_constraint
from jax.experimental.pallas import tpu as pltpu
from jax.sharding import PartitionSpec as P

D = 1152
HD = 72
FF = 3072
STEP = 10


EPSILON = 1e-06
NEG_FILL = -1e30
PRECISE = lax.Precision.HIGHEST
BETA_FIRST = 0.9
BETA_SECOND = 0.95
ADAM_EPSILON = 1e-08
DECAY_RATE = 0.01
SMALL_RATE = 0.5


def rms_scaled(values):
    return values * lax.rsqrt(jnp.mean(values * values, axis=-1, keepdims=True) + EPSILON)


def modulate_in(base_rows, scale_rows, shift_rows):
    return rms_scaled(base_rows) * (1.0 + scale_rows) + shift_rows


def time_embed(step_ids, width):
    half_width = width // 2
    frequency = jnp.exp(-math.log(10000.0) * jnp.arange(half_width, dtype=jnp.float32) / half_width)
    angles = step_ids.astype(jnp.float32)[..., None] * frequency
    return jnp.concatenate([jnp.cos(angles), jnp.sin(angles)], axis=-1)


def layout(item_lengths, item_widths, row_index):
    ends_at = jnp.cumsum(item_lengths)
    starts_at = ends_at - item_lengths
    segment = jnp.sum((row_index[:, None] >= ends_at[None, :]).astype(jnp.int32), axis=1)
    member = segment[:, None] == jnp.arange(item_lengths.shape[0], dtype=jnp.int32)[None, :]
    offset = jnp.sum(jnp.where(member, starts_at[None, :], 0), axis=1)
    grid_span = jnp.sum(jnp.where(member, item_widths[None, :], 0), axis=1)
    inside = row_index - offset
    return (segment, inside // grid_span, inside % grid_span)


def rope_tables(grid_row, grid_col, head_size):
    quarter = head_size // 4
    frequency = jnp.exp(-math.log(10000.0) * jnp.arange(quarter, dtype=jnp.float32) / quarter)
    row_angle = grid_row.astype(jnp.float32)[:, None] * frequency[None, :]
    col_angle = grid_col.astype(jnp.float32)[:, None] * frequency[None, :]
    return (jnp.cos(row_angle), jnp.sin(row_angle), jnp.cos(col_angle), jnp.sin(col_angle))


def turn_half(part, cosine, sine):
    quarter = part.shape[-1] // 2
    first_part = part[..., :quarter]
    second_part = part[..., quarter:]
    cosine = cosine[:, None, :]
    sine = sine[:, None, :]
    return jnp.concatenate(
        [first_part * cosine - second_part * sine, first_part * sine + second_part * cosine],
        axis=-1,
    )


def rotate(values, tables):
    half_size = values.shape[-1] // 2
    return jnp.concatenate(
        [
            turn_half(values[..., :half_size], tables[0], tables[1]),
            turn_half(values[..., half_size:], tables[2], tables[3]),
        ],
        axis=-1,
    )


def qk_prepare(raw_query, raw_key, gains, tables):
    head_size = gains.shape[1]
    row_count = raw_query.shape[0]
    head_count = raw_query.shape[1] // head_size
    query_norm = rms_scaled(raw_query.reshape(row_count, head_count, head_size)) * gains[0]
    key_norm = rms_scaled(raw_key.reshape(row_count, head_count, head_size)) * gains[1]
    return (rotate(query_norm, tables), rotate(key_norm, tables))


def block_geometry(total_rows):
    query_block = min(512, total_rows)
    return (query_block, total_rows, total_rows // query_block)


def window_start(block_index, query_block, key_window, total_rows):
    return jnp.clip(block_index * query_block - query_block, 0, total_rows - key_window)


def masked_scores(query_low, key_low, segment, block_index, query_block, key_window):
    total_rows = query_low.shape[0]
    scale = query_low.shape[2] ** (-0.5)
    query_start = block_index * query_block
    key_start = window_start(block_index, query_block, key_window, total_rows)
    queries = lax.dynamic_slice_in_dim(query_low, query_start, query_block, 0)
    seg_query = lax.dynamic_slice_in_dim(segment, query_start, query_block, 0)
    scores = (
        jnp.einsum("qhe,khe->hqk", queries, key_low, preferred_element_type=jnp.float32) * scale
    )
    allowed = (seg_query[:, None] == segment[None, :])[None]
    return (jnp.where(allowed, scores, NEG_FILL), queries, key_low, query_start, key_start)


def attend(query_low, key_low, value_low, segment):
    total_rows = query_low.shape[0]
    query_block, key_window, block_count = block_geometry(total_rows)

    def one_block(block_index):
        scores, queries, keyset, query_start, key_start = masked_scores(
            query_low, key_low, segment, block_index, query_block, key_window
        )
        peak = jnp.max(scores, axis=-1, keepdims=True)
        expo = jnp.exp(scores - peak)
        total_exp = jnp.sum(expo, axis=-1, keepdims=True)
        probs = (expo / total_exp).astype(jnp.bfloat16)
        result = jnp.einsum("hqk,khe->qhe", probs, value_low, preferred_element_type=jnp.float32)
        return (result, (peak + jnp.log(total_exp))[..., 0])

    outputs, log_sums = lax.map(one_block, jnp.arange(block_count, dtype=jnp.int32))
    return (outputs.reshape(total_rows, query_low.shape[1], query_low.shape[2]), log_sums)


def attend_back(query_low, key_low, value_low, d_attn, log_sums, segment):
    total_rows = query_low.shape[0]
    query_block, key_window, block_count = block_geometry(total_rows)
    scale = query_low.shape[2] ** (-0.5)
    zeros_like = jnp.zeros(query_low.shape, jnp.float32)

    def one_block(carry, block_index):
        d_keys, d_values = carry
        scores, queries, keyset, query_start, key_start = masked_scores(
            query_low, key_low, segment, block_index, query_block, key_window
        )
        grads_block = lax.dynamic_slice_in_dim(d_attn, query_start, query_block, 0)
        probs = jnp.exp(scores - log_sums[block_index][:, :, None])
        low_probs = probs.astype(jnp.bfloat16)
        d_probs = jnp.einsum(
            "qhe,khe->hqk", grads_block, value_low, preferred_element_type=jnp.float32
        )
        row_dot = jnp.sum(probs * d_probs, axis=-1, keepdims=True)
        d_scores = (probs * (d_probs - row_dot)).astype(jnp.bfloat16)
        d_query = (
            jnp.einsum("hqk,khe->qhe", d_scores, keyset, preferred_element_type=jnp.float32) * scale
        )
        d_key_part = (
            jnp.einsum("hqk,qhe->khe", d_scores, queries, preferred_element_type=jnp.float32)
            * scale
        )
        d_value_part = jnp.einsum(
            "hqk,qhe->khe", low_probs, grads_block, preferred_element_type=jnp.float32
        )
        d_keys = d_keys + d_key_part
        d_values = d_values + d_value_part
        return ((d_keys, d_values), d_query)

    (d_keys, d_values), d_queries = lax.scan(
        one_block, (zeros_like, zeros_like), jnp.arange(block_count, dtype=jnp.int32)
    )
    return (d_queries.reshape(query_low.shape), d_keys, d_values)


def adam_update(weight, first_moment, second_moment, gradient, rate, clip):
    clipped = gradient * clip
    new_first = BETA_FIRST * first_moment + (1.0 - BETA_FIRST) * clipped
    new_second = BETA_SECOND * second_moment + (1.0 - BETA_SECOND) * clipped * clipped
    unbiased_first = new_first / (1.0 - BETA_FIRST**STEP)
    unbiased_second = new_second / (1.0 - BETA_SECOND**STEP)
    new_weight = weight - rate * (
        unbiased_first / (jnp.sqrt(unbiased_second) + ADAM_EPSILON) + DECAY_RATE * weight
    )
    return (new_weight, new_first, new_second)


ZSIDE = 4
CORES = 2


def place_of(rank, count):
    xside = count // (ZSIDE * CORES)
    return (rank // (xside * CORES), (rank // CORES) % xside, rank % CORES)


def shift_pairs(count, dim, amount):
    xside = count // (ZSIDE * CORES)
    pairs = []
    for rank in range(count):
        z, x, core = place_of(rank, count)
        if dim == "z":
            z = (z + amount) % ZSIDE
        elif dim == "x":
            x = (x + amount) % xside
        else:
            core = (core + amount) % CORES
        pairs.append((rank, (z * xside + x) * CORES + core))
    return pairs


def send(values, dim, amount):
    count = lax.axis_size("dp")
    return lax.ppermute(values, "dp", shift_pairs(count, dim, amount))


def tensor_send(values, amount):
    count = lax.axis_size("tensor")
    return lax.ppermute(values, "tensor", [(r, (r + amount) % count) for r in range(count)])


def block_order(rank, count):
    xside = count // (ZSIDE * CORES)
    z, x, core = place_of(rank, count)
    flips = jnp.arange(CORES, dtype=jnp.int32)[:, None, None]
    turns = jnp.arange(xside, dtype=jnp.int32)[None, :, None]
    hops = jnp.arange(ZSIDE, dtype=jnp.int32)[None, None, :]
    their_z = (z - hops) % ZSIDE
    their_x = (x - turns) % xside
    their_core = (core + flips) % CORES
    return ((their_z * xside + their_x) * CORES + their_core).reshape(count)


def near_rows(shard):
    return jnp.concatenate([shard] + [send(shard, "z", hop) for hop in range(1, ZSIDE)], axis=0)


def far_rows(near):
    xside = lax.axis_size("dp") // (ZSIDE * CORES)
    mine = jnp.concatenate([near] + [send(near, "x", turn) for turn in range(1, xside)], axis=0)
    return jnp.concatenate([mine, send(mine, "core", 1)], axis=0)


def gather_rows(shard):
    return far_rows(near_rows(shard))


def by_rows(values):
    return with_layout_constraint(values, Layout(tuple(range(values.ndim))))


def gated(value, gate):
    return lax.optimization_barrier((value, gate))


def fold_core(mine, other):
    parts = []
    for own, theirs in zip(mine, other):
        came = send(theirs, "core", 1)
        parts.append((own.astype(jnp.float32) + came.astype(jnp.float32)).astype(own.dtype))
    return parts


def fold_x(parts):
    z = place_of(lax.axis_index("dp"), lax.axis_size("dp"))[0]
    total = parts[0].astype(jnp.float32)
    for turn in range(1, len(parts)):
        total = total + send(parts[turn], "x", -turn).astype(jnp.float32)
    total = total.astype(parts[0].dtype)
    return [
        lax.dynamic_index_in_dim(total, (z - hop) % ZSIDE, 0, keepdims=False) for hop in range(ZSIDE)
    ]


def fold_z(cuts):
    total = cuts[0].astype(jnp.float32)
    for hop in range(1, ZSIDE):
        total = total + send(cuts[hop], "z", -hop).astype(jnp.float32)
    return total


def reduce_rows(mine, other):
    xside = lax.axis_size("dp") // (ZSIDE * CORES)
    total = mine + send(other, "core", 1)
    for side, count in (("x", xside), ("z", ZSIDE)):
        rows = total.shape[0] // count
        cuts = [total[turn * rows : (turn + 1) * rows] for turn in range(count)]
        total = cuts[0]
        for turn in range(1, count):
            total = total + send(cuts[turn], side, -turn)
    return total


def split_core(gradient):
    count = lax.axis_size("dp")
    xside = count // (ZSIDE * CORES)
    z, x, core = place_of(lax.axis_index("dp"), count)
    rows = gradient.shape[0] // count
    blocks = gradient.reshape(ZSIDE, xside, CORES, rows, -1)
    halves = []
    for side in (core, 1 - core):
        half = lax.dynamic_index_in_dim(blocks, side, 2, keepdims=False)
        turns = [(x - turn) % xside for turn in range(xside)]
        cut = [lax.dynamic_index_in_dim(half, turn, 1, keepdims=False) for turn in turns]
        halves.append(cut)
    return halves


def tensor_gather(values):
    count = lax.axis_size("tensor")
    return jnp.concatenate([values] + [tensor_send(values, hop) for hop in range(1, count)], axis=0)


def tensor_reduce(values):
    count = lax.axis_size("tensor")
    rows = values.shape[0] // count
    total = values[:rows].astype(jnp.float32)
    for hop in range(1, count):
        came = tensor_send(values[hop * rows : (hop + 1) * rows], -hop)
        total = total + came.astype(jnp.float32)
    return total


def tensor_total(values):
    count = lax.axis_size("tensor")
    if count == 2:
        half = values.shape[0] // 2
        came = tensor_send(values, 1)
        came = jnp.concatenate([came[half:], came[:half]], axis=0)
        return values.astype(jnp.float32) + came.astype(jnp.float32)
    return tensor_gather(tensor_reduce(values).astype(values.dtype)).astype(jnp.float32)


def everywhere_sum(values):
    for axis in ("dp", "tensor"):
        count = lax.axis_size(axis)
        step = 1
        while step < count:
            values = values + lax.ppermute(values, axis, [(r, r ^ step) for r in range(count)])
            step *= 2
    return values


def mlp_kernel(rows_ref, grad_ref, held, out_ref, in_ref, act_ref, out_acc, in_acc):
    step = pl.program_id(0)
    width = held.shape[1] // 3
    gate_w = held[:, :width]
    up_w = held[:, width : 2 * width]
    down_w = held[:, 2 * width :]

    @pl.when(step == 0)
    def _():
        out_acc[...] = jnp.zeros_like(out_acc)
        in_acc[...] = jnp.zeros_like(in_acc)

    across = (((1,), (1,)), ((), ()))
    gate = jnp.dot(rows_ref[...], gate_w, preferred_element_type=jnp.float32)
    up = jnp.dot(rows_ref[...], up_w, preferred_element_type=jnp.float32)
    d_hidden = jnp.dot(grad_ref[...], down_w, preferred_element_type=jnp.float32)
    sigmoid = 1.0 / (1.0 + jnp.exp(-gate))
    silu = gate * sigmoid
    hidden = (silu * up).astype(jnp.bfloat16)
    d_gate = (d_hidden * up * sigmoid * (1.0 + gate * (1.0 - sigmoid))).astype(jnp.bfloat16)
    d_up = (d_hidden * silu).astype(jnp.bfloat16)
    act_ref[:, :width] = d_gate
    act_ref[:, width : 2 * width] = d_up
    act_ref[:, 2 * width :] = hidden
    out_acc[...] += lax.dot_general(hidden, down_w, across, preferred_element_type=jnp.float32)
    in_acc[...] += lax.dot_general(
        d_gate, gate_w, across, preferred_element_type=jnp.float32
    ) + lax.dot_general(d_up, up_w, across, preferred_element_type=jnp.float32)

    @pl.when(step == pl.num_programs(0) - 1)
    def _():
        out_ref[...] = out_acc[...].astype(out_ref.dtype)
        in_ref[...] = in_acc[...].astype(in_ref.dtype)


def mlp_part(rows, grad, weights, blocks):
    count, width = rows.shape
    columns = weights.shape[1]
    block = columns // blocks
    whole = pl.BlockSpec((count, width), lambda i: (0, 0))
    across = pl.BlockSpec((width, block), lambda i: (0, i))
    acts = pl.BlockSpec((count, block), lambda i: (0, i))
    return pl.pallas_call(
        mlp_kernel,
        grid=(blocks,),
        in_specs=[whole, whole, across],
        out_specs=[whole, whole, acts],
        out_shape=[jax.ShapeDtypeStruct((count, width), jnp.bfloat16)] * 2
        + [jax.ShapeDtypeStruct((count, columns), jnp.bfloat16)],
        scratch_shapes=[pltpu.VMEM((count, width), jnp.float32)] * 2,
        cost_estimate=pl.CostEstimate(
            flops=4 * count * width * columns,
            bytes_accessed=2 * width * columns,
            transcendentals=count * columns // 3,
        ),
        compiler_params=pltpu.CompilerParams(vmem_limit_bytes=60 * 1024 * 1024),
    )(rows, grad, weights)


def grad_kernel(rows_t_ref, grad_t_ref, *refs):
    acts, target = refs[:-1], refs[-1]
    width = target.shape[1] // 3
    for at, left in ((0, rows_t_ref), (width, rows_t_ref), (2 * width, grad_t_ref)):
        cut = slice(at, at + width)
        begin = 0
        product = None
        for act_ref in acts:
            rows = slice(begin, begin + act_ref.shape[0])
            share = jnp.dot(left[:, rows], act_ref[:, cut], preferred_element_type=jnp.float32)
            product = share if product is None else product + share
            begin = rows.stop
        target[:, cut] = product.astype(target.dtype)


def grad_part(rows_t, grad_t, acts, blocks):
    width, count = rows_t.shape
    columns = acts[0].shape[1]
    block = columns // blocks
    whole = pl.BlockSpec((width, count), lambda i: (0, 0))
    return pl.pallas_call(
        grad_kernel,
        grid=(blocks,),
        in_specs=[whole, whole]
        + [pl.BlockSpec((act.shape[0], block), lambda i: (0, i)) for act in acts],
        out_specs=pl.BlockSpec((width, block), lambda i: (0, i)),
        out_shape=jax.ShapeDtypeStruct((width, columns), jnp.bfloat16),
        cost_estimate=pl.CostEstimate(
            flops=2 * count * width * columns, bytes_accessed=2 * width * columns, transcendentals=0
        ),
        compiler_params=pltpu.CompilerParams(vmem_limit_bytes=60 * 1024 * 1024),
    )(rows_t, grad_t, *acts)


def mlp_plain(rows, grad, weights, blocks):
    width = weights.shape[0]
    block = weights.shape[1] // (3 * blocks)
    split = weights.reshape(width, blocks, 3, block)
    gate_w, up_w, down_w = [split[:, :, slot].reshape(width, blocks * block) for slot in range(3)]
    gate = jnp.dot(rows, gate_w, preferred_element_type=jnp.float32)
    up = jnp.dot(rows, up_w, preferred_element_type=jnp.float32)
    d_hidden = jnp.dot(grad, down_w, preferred_element_type=jnp.float32)
    sigmoid = jax.nn.sigmoid(gate)
    hidden = (gate * sigmoid * up).astype(jnp.bfloat16)
    d_gate = (d_hidden * up * sigmoid * (1.0 + gate * (1.0 - sigmoid))).astype(jnp.bfloat16)
    d_up = (d_hidden * gate * sigmoid).astype(jnp.bfloat16)
    out_sum = jnp.dot(hidden, down_w.T, preferred_element_type=jnp.float32)
    in_sum = jnp.dot(d_gate, gate_w.T, preferred_element_type=jnp.float32) + jnp.dot(
        d_up, up_w.T, preferred_element_type=jnp.float32
    )
    grads = [
        jnp.einsum("gd,gf->df", left, right, preferred_element_type=jnp.float32)
        .astype(jnp.bfloat16)
        .reshape(width, blocks, block)
        for left, right in ((rows, d_gate), (rows, d_up), (grad, hidden))
    ]
    packed = jnp.stack(grads, axis=2).reshape(width, 3 * blocks * block)
    return (out_sum.astype(jnp.bfloat16), in_sum.astype(jnp.bfloat16), packed)


def pack_attn_kernel(qkv_ref, out_ref, target):
    columns = out_ref.shape[1]
    for slot in range(3):
        target[:, slot * columns : (slot + 1) * columns] = qkv_ref[slot].astype(target.dtype)
    target[:, 3 * columns :] = out_ref[...].astype(target.dtype)


def pack_attn(qkv, out):
    rows, columns = out.shape
    return pl.pallas_call(
        pack_attn_kernel, out_shape=jax.ShapeDtypeStruct((rows, 4 * columns), jnp.bfloat16)
    )(qkv, out)


def pack_mlp_kernel(block, gateup_ref, down_ref, target):
    for begin in range(0, down_ref.shape[1], block):
        cut = slice(begin, begin + block)
        at = 3 * begin
        target[:, at : at + block] = gateup_ref[0, :, cut].astype(target.dtype)
        target[:, at + block : at + 2 * block] = gateup_ref[1, :, cut].astype(target.dtype)
        target[:, at + 2 * block : at + 3 * block] = down_ref[:, cut].astype(target.dtype)


def pack_mlp(gateup, down, block):
    rows, hidden = down.shape
    return pl.pallas_call(
        partial(pack_mlp_kernel, block),
        out_shape=jax.ShapeDtypeStruct((rows, 3 * hidden), jnp.bfloat16),
    )(gateup, down)


def mod_kernel(stride, rows_ref, ada_ref, target):
    columns = ada_ref.shape[2]
    target[...] = jnp.zeros_like(target)
    for slot in range(ada_ref.shape[0]):
        target[:, slot * stride : slot * stride + columns] = jnp.dot(
            rows_ref[...], ada_ref[slot].astype(jnp.bfloat16), preferred_element_type=jnp.float32
        )


def mod_product(rows, ada, stride):
    return pl.pallas_call(
        partial(mod_kernel, stride),
        out_shape=jax.ShapeDtypeStruct((rows.shape[0], ada.shape[0] * stride), jnp.float32),
    )(rows, ada)


def adam_kernel(rates, clip_ref, *refs):
    clip = clip_ref[0, 0]
    count = len(rates)
    grads, states, targets = refs[:count], refs[count : 4 * count], refs[4 * count :]
    for index, rate in enumerate(rates):
        held = states[3 * index : 3 * index + 3]
        put = targets[3 * index : 3 * index + 3]
        paired = len(grads[index].shape) == 3 and grads[index].shape[1] == 2
        rows = grads[index].shape[0 if paired else -2]
        tall = 8 if rows % 8 == 0 else rows

        def step(
            at, carry, held=held, put=put, source=grads[index], rate=rate, tall=tall, paired=paired
        ):
            cut = pl.ds(at * tall, tall)
            cell = (cut,) if paired or len(source.shape) == 2 else (slice(None), cut)
            result = adam_update(*[ref[cell] for ref in held], source[cell], rate, clip)
            for ref, value in zip(put, result):
                ref[cell] = value
            return carry

        lax.fori_loop(0, rows // tall, step, 0)


def adam_all(clip, grads, states, rates, row_share):
    steps = 3 if row_share % 24 == 0 else 1

    def spec_of(values):
        shape = values.shape
        if row_share not in shape[:-1]:
            return pl.BlockSpec(shape, lambda i: (0,) * len(shape))
        dim = shape.index(row_share)
        block = tuple(size // steps if at == dim else size for at, size in enumerate(shape))
        return pl.BlockSpec(
            block, lambda i: tuple(i if at == dim else 0 for at in range(len(shape)))
        )

    return pl.pallas_call(
        partial(adam_kernel, rates),
        grid=(steps,),
        in_specs=[pl.BlockSpec(memory_space=pltpu.SMEM)] + [spec_of(x) for x in grads + states],
        out_specs=[spec_of(x) for x in states],
        out_shape=[jax.ShapeDtypeStruct(x.shape, x.dtype) for x in states],
        compiler_params=pltpu.CompilerParams(vmem_limit_bytes=60 * 1024 * 1024),
    )(clip.reshape(1, 1), *grads, *states)


def padded(columns):
    return -(-columns // 128) * 128


def local(
    tokens,
    cotangent,
    lengths,
    grid_width,
    timestep,
    class_id,
    class_table,
    ada_weight,
    ada_m,
    ada_v,
    ada_bias,
    bias_m,
    bias_v,
    qkv_weight,
    qkv_m,
    qkv_v,
    out_weight,
    out_m,
    out_v,
    gateup_weight,
    gateup_m,
    gateup_v,
    down_weight,
    down_m,
    down_v,
    qk_gain,
    gain_m,
    gain_v,
):
    tensor_count = lax.axis_size("tensor")
    data_count = lax.axis_size("dp")
    tensor_rank = lax.axis_index("tensor")
    data_rank = lax.axis_index("dp")
    local_rows, model_width = tokens.shape
    group_rows = local_rows * tensor_count
    column_share = model_width // tensor_count
    row_share = ada_weight.shape[0]
    head_size = qk_gain.shape[1]
    item_count = lengths.shape[1]
    class_count = class_table.shape[0]
    hidden_share = down_weight.shape[1]
    bf16 = jnp.bfloat16

    stride = padded(column_share)
    block = 256 if hidden_share % 512 == 0 else hidden_share
    blocks = hidden_share // block
    swap = lambda values: jnp.transpose(values, (1, 0, 2))
    attn_shard = pack_attn(swap(qkv_weight), out_weight)
    full_attn = lax.all_gather(attn_shard, "dp", axis=0, tiled=True)
    mlp_shard = pack_mlp(swap(gateup_weight), down_weight, block)
    full_mlp = lax.all_gather(mlp_shard, "dp", axis=0, tiled=True)
    full_qkv = full_attn[:, : 3 * column_share]
    full_out = full_attn[:, 3 * column_share :]

    ids = gather_rows(jnp.stack([class_id[0], timestep[0]])[None])
    item_ids = ids[:, 0].reshape(-1)
    item_steps = ids[:, 1].reshape(-1)
    class_onehot = (
        item_ids[:, None] == jnp.arange(class_count, dtype=jnp.int32)[None, :]
    ).astype(bf16)
    condition = jnp.dot(class_onehot, class_table, preferred_element_type=jnp.float32) + time_embed(
        item_steps, model_width
    )
    silu_all = jax.nn.silu(condition).astype(bf16)
    silu_own = lax.dynamic_slice_in_dim(silu_all, data_rank * row_share, row_share, 1)
    mod_part = mod_product(silu_own, swap(ada_weight), stride)
    half_items = data_count * item_count // 2
    mod_share = reduce_rows(mod_part[:half_items], mod_part[half_items:])
    mod_share = mod_share.reshape(item_count, 6, stride)[:, :, :column_share]
    bias_share = lax.dynamic_slice_in_dim(ada_bias, tensor_rank * column_share, column_share, 1)
    mod_share = mod_share + bias_share[None]
    if tensor_count == 2:
        mod_other = tensor_send(mod_share, 1)
        lower = jnp.where(tensor_rank == 0, mod_share, mod_other)
        upper = jnp.where(tensor_rank == 0, mod_other, mod_share)
        modulation = jnp.concatenate([lower, upper], axis=2)
    else:
        modulation = lax.all_gather(mod_share, "tensor", axis=2, tiled=True)
    tokens_all = by_rows(tensor_gather(tokens))
    cot_all = by_rows(tensor_gather(cotangent))
    base_rows = tokens_all.astype(jnp.float32)
    row_blocks = (tensor_rank - jnp.arange(tensor_count, dtype=jnp.int32)) % tensor_count
    row_index = (
        row_blocks[:, None] * local_rows + jnp.arange(local_rows, dtype=jnp.int32)[None, :]
    ).reshape(-1)
    segment, grid_row, grid_col = layout(lengths[0], grid_width[0], row_index)
    tables = rope_tables(grid_row, grid_col, head_size)

    def mod_rows(slot, count):
        picked = modulation[0, slot][None, :]
        for item in range(1, item_count):
            picked = jnp.where(
                segment[:count, None] == item, modulation[item, slot][None, :], picked
            )
        return picked

    def mod_sums(values):
        own = segment[:local_rows]
        return jnp.stack(
            [
                jnp.sum(jnp.where(own[:, None] == item, values, 0.0), axis=0)
                for item in range(item_count)
            ]
        )

    attn_in = modulate_in(base_rows, mod_rows(1, group_rows), mod_rows(0, group_rows))
    attn_in = by_rows(attn_in.astype(bf16))
    qkv_raw = jnp.dot(attn_in, full_qkv, preferred_element_type=jnp.float32)
    raw_query, raw_key, raw_value = [
        qkv_raw[:, slot * column_share : (slot + 1) * column_share] for slot in range(3)
    ]
    query_rot, key_rot = qk_prepare(raw_query, raw_key, qk_gain, tables)
    query_low = query_rot.astype(bf16)
    key_low = key_rot.astype(bf16)
    value_low = raw_value.reshape(group_rows, -1, head_size).astype(bf16)
    attn_vals, log_sums = attend(query_low, key_low, value_low, segment)
    attn_low = attn_vals.reshape(group_rows, column_share).astype(bf16)
    branch = jnp.einsum("gc,dc->gd", attn_low, full_out, preferred_element_type=jnp.float32)
    branch, cot_all = gated(by_rows(branch.astype(bf16)), cot_all)
    cot_rows = cot_all.astype(jnp.float32)
    branch = by_rows(tensor_total(branch))
    mid_rows = by_rows(base_rows + mod_rows(2, group_rows) * branch)
    scale_two = mod_rows(4, group_rows)
    mlp_in = by_rows(modulate_in(mid_rows, scale_two, mod_rows(3, group_rows)).astype(bf16))
    gate_two = mod_rows(5, group_rows)
    d_branch_mlp = by_rows((gate_two * cot_rows).astype(bf16))

    if group_rows <= 512:
        turned = (mlp_in.T, d_branch_mlp.T)
        (mlp_in, d_branch_mlp), turned = gated((mlp_in, d_branch_mlp), turned)
        out_part, in_part, acts = mlp_part(mlp_in, d_branch_mlp, full_mlp, blocks)
        g_mlp = grad_part(*turned, (acts,), blocks)
    else:
        out_part, in_part, g_mlp = mlp_plain(mlp_in, d_branch_mlp, full_mlp, blocks)
    sum_mlp = lax.psum_scatter(g_mlp, "dp", scatter_dimension=0, tiled=True)
    d_mlp_in = by_rows(tensor_total(in_part))
    branch_mlp = by_rows(tensor_reduce(out_part))
    out_rows = mid_rows[:local_rows] + gate_two[:local_rows] * branch_mlp
    out_tokens = out_rows.astype(bf16)

    d_mid_norm, d_scale_two, d_shift_two = jax.vjp(
        modulate_in, mid_rows, scale_two, jnp.zeros_like(mid_rows)
    )[1](d_mlp_in)
    d_mid = by_rows(cot_rows + d_mid_norm)
    d_branch_attn = by_rows((mod_rows(2, group_rows) * d_mid).astype(bf16))
    d_attn = jnp.einsum("gd,dc->gc", d_branch_attn, full_out, preferred_element_type=jnp.float32)
    d_attn = d_attn.astype(bf16).reshape(query_low.shape)
    d_query_rot, d_key_rot, d_values = attend_back(
        query_low, key_low, value_low, d_attn, log_sums, segment
    )
    _, pull_qk = jax.vjp(partial(qk_prepare, tables=tables), raw_query, raw_key, qk_gain)
    d_query_raw, d_key_raw, g_gain = pull_qk((d_query_rot, d_key_rot))
    d_qkv_low = jnp.concatenate(
        [d_query_raw, d_key_raw, d_values.reshape(group_rows, -1)], axis=1
    ).astype(bf16)
    g_qkv = jnp.einsum("gd,gc->dc", attn_in, d_qkv_low, preferred_element_type=jnp.float32)
    mine, other = split_core(by_rows(g_qkv.astype(bf16)))
    other, d_qkv_low = gated(other, d_qkv_low)
    d_attn_part = jnp.einsum("gc,dc->gd", d_qkv_low, full_qkv, preferred_element_type=jnp.float32)
    turns, d_attn_part = gated(fold_core(mine, other), by_rows(d_attn_part.astype(bf16)))
    d_attn_in = by_rows(tensor_reduce(d_attn_part))
    turns, d_branch_attn = gated(turns, d_branch_attn)
    g_out = jnp.einsum("gd,gc->dc", d_branch_attn, attn_low, preferred_element_type=jnp.float32)
    out_turns = fold_core(*split_core(by_rows(g_out.astype(bf16))))
    qkv_cuts = fold_x(turns)
    qkv_cuts, (d_attn_in, out_turns) = gated(qkv_cuts, (d_attn_in, out_turns))
    sum_qkv = fold_z(qkv_cuts)
    out_cuts = fold_x(out_turns)

    own_scale = mod_rows(1, local_rows)
    d_base_norm, d_scale_one, d_shift_one = jax.vjp(
        modulate_in, base_rows[:local_rows], own_scale, jnp.zeros_like(own_scale)
    )[1](d_attn_in)
    input_grad = (d_mid[:local_rows] + d_base_norm).astype(bf16)
    d_mod_part = jnp.stack(
        [
            mod_sums(d_shift_one),
            mod_sums(d_scale_one),
            mod_sums(d_mid[:local_rows] * branch[:local_rows]),
            mod_sums(d_shift_two[:local_rows]),
            mod_sums(d_scale_two[:local_rows]),
            mod_sums(cot_rows[:local_rows] * branch_mlp),
        ],
        axis=1,
    )
    d_mod_part, out_cuts = gated(d_mod_part, out_cuts)
    sum_out = fold_z(out_cuts)
    if tensor_count == 2:
        lower, upper = d_mod_part[:, :, :column_share], d_mod_part[:, :, column_share:]
        theirs = jnp.where(tensor_rank == 0, upper, lower)
        d_mod = jnp.where(tensor_rank == 0, lower, upper) + tensor_send(theirs, 1)
    else:
        d_mod = lax.psum_scatter(d_mod_part, "tensor", scatter_dimension=2, tiled=True)
    d_mod = jnp.pad(d_mod, ((0, 0), (0, 0), (0, stride - column_share)))
    d_mod_near = near_rows(d_mod.reshape(item_count, 6 * stride))
    d_mod_all = far_rows(d_mod_near)
    sum_ada = lax.dot_general(
        silu_own.astype(jnp.float32),
        d_mod_all,
        (((0,), (0,)), ((), ())),
        precision=PRECISE,
        preferred_element_type=jnp.float32,
    )
    bias_share = jnp.sum(d_mod_all, axis=0).reshape(6, stride)[:, :column_share]
    if tensor_count == 2:
        bias_other = tensor_send(bias_share, 1)
        lower = jnp.where(tensor_rank == 0, bias_share, bias_other)
        upper = jnp.where(tensor_rank == 0, bias_other, bias_share)
        bias_grad = jnp.concatenate([lower, upper], axis=1)
    else:
        bias_grad = lax.all_gather(bias_share, "tensor", axis=1, tiled=True)

    local_squares = jnp.sum(sum_ada * sum_ada) + jnp.sum(sum_qkv * sum_qkv)
    local_squares = local_squares + jnp.sum(bias_share * bias_share) / data_count
    local_squares = local_squares + jnp.sum(sum_out * sum_out)
    local_squares = local_squares + jnp.sum(jnp.square(sum_mlp.astype(jnp.float32)))
    packet = jnp.concatenate(
        [
            g_gain.reshape(-1),
            local_squares[None],
            jnp.zeros((256 - 2 * head_size - 1,), jnp.float32),
        ]
    ).reshape(2, 128)
    packet = everywhere_sum(packet).reshape(-1)
    gain_total = packet[: 2 * head_size].reshape(2, head_size)
    grad_norm = jnp.sqrt(
        packet[2 * head_size] + jnp.sum(gain_total * gain_total)
    )
    tokens_all_count = local_rows * tensor_count * data_count
    params_all = 10 * D * D + 3 * D * FF + 6 * D + 2 * HD
    limit = 0.01 * math.sqrt(tokens_all_count * params_all)
    clip = limit / jnp.maximum(grad_norm, limit)
    matrix_rate = model_width ** (-0.5)

    out_rate = (model_width // 64) ** (-0.5)
    hidden_rate = FF ** (-0.5)
    rates = (matrix_rate, SMALL_RATE, matrix_rate, out_rate, matrix_rate, hidden_rate, SMALL_RATE)
    same = lambda values: values
    views = (
        ((ada_weight, ada_m, ada_v), swap, swap),
        ((ada_bias, bias_m, bias_v), same, same),
        ((qkv_weight, qkv_m, qkv_v), swap, swap),
        ((out_weight, out_m, out_v), same, same),
        ((gateup_weight, gateup_m, gateup_v), same, same),
        ((down_weight, down_m, down_v), same, same),
        ((qk_gain, gain_m, gain_v), same, same),
    )
    by_slot = lambda values, width: jnp.stack(
        [values[:, at : at + column_share] for at in range(0, values.shape[1], width)]
    )
    mlp_split = sum_mlp.reshape(row_share, blocks, 3, block).astype(jnp.float32)
    gateup_grad = jnp.stack(
        [mlp_split[:, :, slot].reshape(row_share, hidden_share) for slot in range(2)], axis=1
    )
    grads = [
        by_slot(sum_ada, stride),
        bias_grad,
        by_slot(sum_qkv, column_share),
        sum_out,
        gateup_grad,
        mlp_split[:, :, 2].reshape(row_share, hidden_share),
        gain_total,
    ]
    states = [view(x) for group, view, _ in views for x in group]
    updated = adam_all(clip, grads, states, rates, row_share)
    updated = [
        back(updated[3 * index + slot])
        for index, (_, _, back) in enumerate(views)
        for slot in range(3)
    ]
    return (
        out_tokens,
        input_grad,
        grad_norm,
        *updated,
    )


def solution(mesh):
    in_specs = (
        P(("dp", "tensor"), None),
        P(("dp", "tensor"), None),
        P("dp", None),
        P("dp", None),
        P("dp", None),
        P("dp", None),
        P(),
        P("dp", None, "tensor"),
        P("dp", None, "tensor"),
        P("dp", None, "tensor"),
        P(),
        P(),
        P(),
        P("dp", None, "tensor"),
        P("dp", None, "tensor"),
        P("dp", None, "tensor"),
        P("dp", "tensor"),
        P("dp", "tensor"),
        P("dp", "tensor"),
        P("dp", None, "tensor"),
        P("dp", None, "tensor"),
        P("dp", None, "tensor"),
        P("dp", "tensor"),
        P("dp", "tensor"),
        P("dp", "tensor"),
        P(),
        P(),
        P(),
    )
    out_specs = (
        P(("dp", "tensor"), None),
        P(("dp", "tensor"), None),
        P(),
        P("dp", None, "tensor"),
        P("dp", None, "tensor"),
        P("dp", None, "tensor"),
        P(),
        P(),
        P(),
        P("dp", None, "tensor"),
        P("dp", None, "tensor"),
        P("dp", None, "tensor"),
        P("dp", "tensor"),
        P("dp", "tensor"),
        P("dp", "tensor"),
        P("dp", None, "tensor"),
        P("dp", None, "tensor"),
        P("dp", None, "tensor"),
        P("dp", "tensor"),
        P("dp", "tensor"),
        P("dp", "tensor"),
        P(),
        P(),
        P(),
    )
    return jax.shard_map(local, mesh=mesh, in_specs=in_specs, out_specs=out_specs, check_vma=False)
```
